32 devices in a mesh: seq: 16 (over z, y, x), tensor: 2 (over core).
Axes of the slice: x: 2, y: 2, z: 4, core: 2. Of those that a mesh axis runs over, the one named last changes fastest.
Arguments:
- hidden: bfloat16 [2, 4096, 8192], P(None, 'seq', 'tensor'), may hold values from -160 to 160
- norm_gain: bfloat16 [8192], P('tensor'), may hold values from 0.25 to 1.75
- value_weight: bfloat16 [8192], P('tensor'), may hold values from -0.0625 to 0.0625
- rewards: float32 [2, 4096], P(None, 'seq'), may hold values from -6 to 6
- done_flags: int32 [2, 4096], P(None, 'seq'), may hold values 0 or 1
- valid_mask: int32 [2, 4096], P('tensor', 'seq'), may hold values 0 or 1
- new_logprob: float32 [2, 4096], P('tensor', 'seq'), may hold values from -1 to 1
- old_logprob: float32 [2, 4096], P('tensor', 'seq'), may hold values from -1 to 1
- discount: float32 [2], replicated, may hold values from 0.9 to 1
- trace_decay: float32 [2], replicated, may hold values from 0.9 to 1
- bootstrap: float32 [2], replicated, may hold values from -5 to 5
Outputs:
- values: float32 [2, 4096], P('tensor', 'seq')
- white_adv: float32 [2, 4096], P('tensor', 'seq')
- token_loss: float32 [2, 4096], P('tensor', 'seq')
- policy_loss: float32 [], replicated
The draws below stay inside these ranges and needn't reach their ends.
All inputs are finite; a program needn't handle non-finite values. No bound on the sum of `done_flags` or of `valid_mask` on one device may be relied on, other than what follows from the above.
Results may differ from the reference program's by a relative error of at most 0.00035.
Values sent between devices are 32-bit elements; how exact they have to be, the bound alone decides.
A program may use at most 64 MiB of HBM per device.

```python
import math
from functools import partial
import jax
import jax.numpy as jnp
from jax import lax

H = 8192
LEN_DEV = 256
SEQS = 2
LENGTH = 4096


def draw_hidden(key, part):
    k_base, k_cols = jax.random.split(jax.random.fold_in(key, 11), 2)
    base = jax.random.truncated_normal(k_base, -4.0, 4.0, (SEQS, LENGTH, H), jnp.float32)
    columns = jnp.exp(jax.random.uniform(k_cols, (H,), jnp.float32) * math.log(10.0))
    drawn = base * columns
    return drawn.astype(jnp.bfloat16)


def draw_discount(key, part):
    k_main = jax.random.fold_in(key, 23)
    spread = jax.random.uniform(k_main, (SEQS,), jnp.float32, 0.1, 0.5)
    return 1.0 - spread / LENGTH


def draw_trace_decay(key, part):
    k_pick, k_slow, k_fast = jax.random.split(jax.random.fold_in(key, 37), 3)
    quick = jax.random.bernoulli(k_pick, 0.5, (SEQS,))
    slow_rate = 1.0 - jax.random.uniform(k_slow, (SEQS,), jnp.float32, 0.2, 1.0) / LENGTH
    fast_rate = 1.0 - jax.random.uniform(k_fast, (SEQS,), jnp.float32, 0.02, 0.033)
    return jnp.where(quick, fast_rate, slow_rate)


def touch_ends(entries, stream_key, low, largest):
    index_at = [jax.random.randint(jax.random.fold_in(stream_key, axis), (), 0, length) for axis, length in enumerate(entries.shape)]
    longest = entries.shape.index(max(entries.shape))
    beside = index_at[:longest] + [(index_at[longest] + 1) % entries.shape[longest]] + index_at[longest + 1:]
    return entries.at[tuple(index_at)].set(low).at[tuple(beside)].set(largest)


def block_scale(own_key, extent, shards, smallest, high):
    factor_of = 1.0
    for position, parts in shards:
        steps = jax.random.uniform(jax.random.fold_in(jax.random.fold_in(own_key, 6), position), (parts,), jnp.float32, smallest / len(shards), high / len(shards))
        factor_of = factor_of * jnp.repeat(jnp.exp(steps), extent[position] // parts).reshape((-1,) + (1,) * (len(extent) - 1 - position))
    return factor_of


def noise(key, dims, deviation, limit, shards=(), held_as=jnp.bfloat16):
    values = deviation * jax.random.normal(key, dims, jnp.float32)
    if shards:
        values = values * block_scale(key, dims, shards, -0.22, 0.18)
    return jnp.clip(values, -limit, limit).astype(held_as)


def setup_inputs(seed: int = 0) -> dict:
    seeds = jax.random.split(jax.random.key(seed), 12)
    return {
        "hidden": draw_hidden(jax.random.fold_in(seeds[11], 71), 0),
        "norm_gain": jnp.clip(1.0 + 0.15 * jax.random.normal(seeds[1], (H,), jnp.float32), 0.25, 1.75).astype(jnp.bfloat16),
        "value_weight": noise(seeds[2], (H,), H ** -0.5, 0.0625, ((0, 2),)),
        "rewards": noise(seeds[3], (SEQS, LENGTH), 1.0, 6.0, ((1, 16),), jnp.float32),
        "done_flags": touch_ends((jax.random.randint(seeds[4], (SEQS, LENGTH), 0, 128 * LEN_DEV) < 1).astype(jnp.int32), jax.random.fold_in(seeds[4], 1), 0, 1),
        "valid_mask": touch_ends((jax.random.randint(seeds[5], (SEQS, LENGTH), 0, 4) < 3).astype(jnp.int32), jax.random.fold_in(seeds[5], 1), 0, 1),
        "new_logprob": noise(seeds[6], (SEQS, LENGTH), 0.15, 1.0, ((0, 2), (1, 16)), jnp.float32),
        "old_logprob": noise(seeds[7], (SEQS, LENGTH), 0.15, 1.0, ((0, 2), (1, 16)), jnp.float32),
        "discount": draw_discount(jax.random.fold_in(seeds[11], 71), 0),
        "trace_decay": draw_trace_decay(jax.random.fold_in(seeds[11], 71), 0),
        "bootstrap": noise(seeds[10], (SEQS,), 1.0, 5.0, (), jnp.float32),
    }


EPS_NORM = 1e-06
EPS_WHITE = 1e-08
CLIP = 0.2

def head_block(scaled, block):
    wide = block.astype(jnp.float32)
    squares = lax.optimization_barrier(jnp.sum(wide * wide, axis=-1))
    products = jnp.dot(wide, scaled, precision=lax.Precision.HIGHEST)
    return products * lax.rsqrt(squares / H + EPS_NORM)

def backward_step(carry, inputs):
    delta_now, coef_now = inputs
    fresh = delta_now + coef_now * carry
    return (fresh, fresh)

def reference(hidden, norm_gain, value_weight, rewards, done_flags, valid_mask, new_logprob, old_logprob, discount, trace_decay, bootstrap):
    scaled = norm_gain.astype(jnp.float32) * value_weight.astype(jnp.float32)
    blocks = hidden.reshape(SEQS * LENGTH // LEN_DEV, LEN_DEV, H)
    values = lax.map(partial(head_block, scaled), blocks).reshape(SEQS, LENGTH)
    alive = 1.0 - done_flags.astype(jnp.float32)
    following = jnp.concatenate([values[:, 1:], bootstrap[:, None]], axis=1)
    delta = rewards + discount[:, None] * alive * following - values
    decay = discount * trace_decay
    coefs = decay[:, None] * alive
    start = jnp.zeros((SEQS,), jnp.float32)
    _, stacked = lax.scan(backward_step, start, (delta.T, coefs.T), reverse=True)
    advantages = stacked.T
    weight = valid_mask.astype(jnp.float32)
    count = jnp.sum(weight)
    mean = jnp.sum(weight * advantages) / count
    variance = jnp.sum(weight * (advantages - mean) ** 2) / count
    white_adv = (advantages - mean) * lax.rsqrt(variance + EPS_WHITE)
    ratio = jnp.exp(new_logprob - old_logprob)
    surrogate = jnp.minimum(ratio * white_adv, jnp.clip(ratio, 1.0 - CLIP, 1.0 + CLIP) * white_adv)
    token_loss = -weight * surrogate
    policy_loss = jnp.sum(token_loss) / count
    return (values, white_adv, token_loss, policy_loss)
```

```python
import functools

import jax
import jax.numpy as jnp
from jax import lax
from jax.experimental import pallas as pl
from jax.experimental.pallas import tpu as pltpu
from jax.sharding import PartitionSpec as P

EPS_NORM = 1e-06
EPS_WHITE = 1e-08
CLIP = 0.2
LANES = 128
BLOCK = 32
UNROLLED = 64
AHEAD_ROWS = 2


def split(parts, count):
    pieces = []
    for _ in range(count):
        pieces.append(parts.astype(jnp.bfloat16))
        parts = parts - pieces[-1].astype(jnp.float32)
    return pieces


def lane_sums(ones, pieces):
    return lax.dot_general(
        ones,
        jnp.concatenate(pieces, axis=1),
        (((1,), (1,)), ((), ())),
        preferred_element_type=jnp.float32,
    )


def kernel(
    seq_count,
    tensor_count,
    width,
    chunk,
    hidden_hbm,
    gain_hbm,
    weight_hbm,
    rewards_hbm,
    flags_hbm,
    mask_hbm,
    new_hbm,
    old_hbm,
    discount_hbm,
    trace_hbm,
    boot_hbm,
    values_ref,
    white_ref,
    token_ref,
    loss_ref,
    hid,
    gain,
    wgt,
    rew,
    flg,
    msk,
    newp,
    oldp,
    disc,
    trc,
    boot,
    ruler,
    scaled,
    parts,
    reach,
    part_send,
    part_recv,
    board,
    carry,
    slope,
    hid_sem,
    near_sem,
    far_sem,
    scalar_sem,
    part_send_sem,
    part_recv_sem,
    send_sem,
    early_recv_sem,
    late_recv_sem,
):
    seqs_all, length, local_width = hid.shape
    own_rows = seqs_all // tensor_count
    devices = seq_count * tensor_count
    chunks = length // chunk
    me_seq = lax.axis_index("seq")
    me_ten = lax.axis_index("tensor")
    first_row = me_ten * own_rows
    my_slot = me_ten * seq_count + me_seq
    early_lanes = pl.ds(0, 2 * length + LANES)
    late_lanes = pl.ds(2 * length + LANES, length + LANES)
    weight_lanes = pl.ds(length, length)
    done_lanes = pl.ds(2 * length, LANES)
    adv_lanes = pl.ds(2 * length + LANES, length)
    offset_lanes = pl.ds(3 * length + LANES, LANES)

    near = [(gain_hbm, gain), (weight_hbm, wgt), (flags_hbm, flg)]
    scalars = [(discount_hbm, disc), (trace_hbm, trc), (boot_hbm, boot)]
    far = [(rewards_hbm, rew), (mask_hbm, msk), (new_hbm, newp), (old_hbm, oldp)]

    def wait_group(group, sem):
        size = sum(dst.size * dst.dtype.itemsize for _, dst in group)
        view = ruler.at[pl.ds(0, size // (4 * LANES))]
        pltpu.make_async_copy(view, view, sem).wait()

    ahead_rows = hid_sem.shape[0] // chunks

    def hid_copy(i, c):
        row = lax.rem(first_row + own_rows + i, seqs_all)
        rows = pl.ds(c * chunk, chunk)
        sem = hid_sem.at[i % ahead_rows * chunks + c]
        return pltpu.make_async_copy(hidden_hbm.at[row, rows, :], hid.at[i, rows, :], sem)

    for src, dst in near:
        pltpu.make_async_copy(src, dst, near_sem).start()
    for src, dst in far:
        pltpu.make_async_copy(src, dst, far_sem).start()
    scalar_copies = [
        pltpu.make_async_copy(src, dst, scalar_sem.at[i]) for i, (src, dst) in enumerate(scalars)
    ]
    for copy in scalar_copies:
        copy.start()
    def prefetch(i, _):
        for c in range(chunks):
            hid_copy(i, c).start()
        return 0

    lax.fori_loop(0, ahead_rows, prefetch, 0)

    barrier = pltpu.get_barrier_semaphore()
    bits = seq_count.bit_length() - 1
    unrolled = devices <= UNROLLED
    mirrored = unrolled and seq_count == 1 << bits
    flips = [(1 << i) * (1 - 2 * lax.rem(lax.div(me_seq, 1 << i), 2)) for i in range(bits)]

    def peer(k):
        if not mirrored:
            slot = lax.rem(my_slot + k, devices)
            return (lax.rem(slot, seq_count), lax.div(slot, seq_count))
        far, turn = divmod(devices - k, tensor_count)
        seq = me_seq
        for i in range(bits):
            if far >> i & 1:
                seq = seq + flips[i]
        return (seq, lax.rem(me_ten + turn, tensor_count))

    def each_peer(act):
        if unrolled:
            for k in range(1, devices):
                act(k, 0)
        else:
            lax.fori_loop(1, devices, act, 0)

    def greet(k, _):
        pl.semaphore_signal(
            barrier, inc=1, device_id=peer(k), device_id_type=pl.DeviceIdType.MESH
        )
        return 0

    each_peer(greet)

    wait_group(near, near_sem)
    for copy in scalar_copies:
        copy.wait()

    for j in range(local_width // LANES):
        cols = pl.ds(j * LANES, LANES)
        row = gain[cols].astype(jnp.float32) * wgt[cols].astype(jnp.float32)
        scaled[:, cols] = jnp.broadcast_to(row.reshape(1, LANES), (8, LANES))

    lane = lax.broadcasted_iota(jnp.int32, (8, length), 1).astype(jnp.float32)
    after = lax.broadcasted_iota(jnp.int32, (BLOCK, length), 1).astype(jnp.float32)
    before = lax.broadcasted_iota(jnp.int32, (BLOCK, length), 0).astype(jnp.float32)

    def coef_of(last_done, row):
        shape = last_done.shape[:-1] + (length,)
        at = lax.broadcasted_iota(jnp.int32, shape, len(shape) - 1).astype(jnp.float32)
        discount = jnp.full(shape, disc[row], jnp.float32)
        decay = discount * jnp.full(shape, trc[row], jnp.float32)
        power = jnp.exp((length - 1.0 - at) * jnp.log(decay))
        return jnp.where(at > last_done[..., 0:1], discount * power, 0.0)

    rows_info = []
    for r in range(own_rows):
        trace = jnp.full((8, length), trc[first_row + r], jnp.float32)
        decay = jnp.full((BLOCK, length), disc[first_row + r], jnp.float32) * trace[0, 0]
        log_decay = jnp.log(decay)
        flags = jnp.broadcast_to(flg[pl.ds(first_row + r, 1), :], (BLOCK, length)) > 0
        last_done = jnp.max(
            jnp.where(flags[0:8, :], lane, -1.0)[0:1, :], axis=1, keepdims=True
        )
        board[my_slot, r : r + 1, done_lanes] = jnp.broadcast_to(last_done, (1, LANES))
        rows_info.append(dict(trace=trace))
        for b in range(length // BLOCK):
            at = before + float(b * BLOCK)
            gap = after - at
            stop = jnp.where(flags & (gap >= 0.0), after, float(length))
            stop = jnp.min(stop, axis=1, keepdims=True)
            reach[r, pl.ds(b * BLOCK, BLOCK), :] = jnp.where(
                (gap >= 0.0) & (after <= stop), jnp.exp(gap * log_decay), 0.0
            )

    def add_chunk(i, c):
        for b in range(chunk // BLOCK):
            rows = pl.ds(c * chunk + b * BLOCK, BLOCK)
            squares = jnp.zeros((BLOCK // 8, 8, LANES), jnp.float32)
            products = jnp.zeros((BLOCK // 8, 8, LANES), jnp.float32)
            for j in range(local_width // LANES):
                cols = pl.ds(j * LANES, LANES)
                x = hid[i, rows, cols].astype(jnp.float32).reshape(BLOCK // 8, 8, LANES)
                squares = squares + x * x
                products = products + x * scaled[:, cols][None]
            parts[i % 2, 0, rows, :] = squares.reshape(BLOCK, LANES)
            parts[i % 2, 1, rows, :] = products.reshape(BLOCK, LANES)

    part_copies = [
        pltpu.make_async_remote_copy(
            src_ref=part_send.at[k - 1],
            dst_ref=part_recv.at[k - 1],
            send_sem=part_send_sem.at[k - 1],
            recv_sem=part_recv_sem.at[k - 1],
            device_id=(me_seq, lax.rem(me_ten + k, tensor_count)),
            device_id_type=pl.DeviceIdType.MESH,
        )
        for k in range(1, tensor_count)
    ]

    def send_all(lanes, recv_sem):
        def send(k, _):
            pltpu.make_async_remote_copy(
                src_ref=board.at[my_slot, :, lanes],
                dst_ref=board.at[my_slot, :, lanes],
                send_sem=send_sem,
                recv_sem=recv_sem,
                device_id=peer(k),
                device_id_type=pl.DeviceIdType.MESH,
            ).start()
            return 0

        each_peer(send)

    def all_blocks(lanes, sem):
        view = board.at[pl.ds(0, devices - 1), :, lanes]
        return pltpu.make_async_copy(view, view, sem)

    def publish():
        wait_group(far, far_sem)
        for r in range(own_rows):
            ratio = jnp.exp(newp[r : r + 1, :] - oldp[r : r + 1, :])
            weight = msk[r : r + 1, :].astype(jnp.float32)
            reward = jnp.broadcast_to(rew[pl.ds(first_row + r, 1), :], (8, length))
            rows_info[r].update(ratio=ratio, weight=weight, reward=reward)
            board[my_slot, r : r + 1, pl.ds(0, length)] = ratio
            board[my_slot, r : r + 1, weight_lanes] = weight
        send_all(early_lanes, early_recv_sem)

    squares_of = [[] for _ in range(seqs_all)]
    products_of = [[] for _ in range(seqs_all)]
    pending = []

    half = lambda axis: lax.broadcasted_iota(jnp.int32, (16, 2 * LANES), axis)
    pick = jnp.where((half(0) < 8) == (half(1) < LANES), 1.0, 0.0).astype(jnp.bfloat16)

    def flush():
        while pending:
            i, start, stop = pending.pop()
            rows = pl.ds(start, stop - start)
            squares = split(parts[i % 2, 0, rows, :], 3)
            products = split(parts[i % 2, 1, rows, :], 3)
            both = sum(lane_sums(pick, pair) for pair in zip(squares, products))
            squares_of[i].append(both[0:8, :])
            products_of[i].append(both[8:16, :])

    partner_rows = seqs_all - own_rows
    group = length
    for i in range(seqs_all):
        start = 0
        for c in range(chunks):
            hid_copy(i, c).wait()
            if i + ahead_rows < seqs_all:
                hid_copy(i + ahead_rows, c).start()
            if i == partner_rows and c == 1:
                publish()
            flush()
            add_chunk(i, c)
            if i > 0 and c == 0 and i <= partner_rows:
                k, r = divmod(i - 1, own_rows)
                squares = jnp.concatenate(squares_of[i - 1], axis=1)
                products = jnp.concatenate(products_of[i - 1], axis=1)
                part_send[k, 2 * r : 2 * r + 1, :] = squares[0:1, :]
                part_send[k, 2 * r + 1 : 2 * r + 2, :] = products[0:1, :]
            if i == partner_rows and c == 0:
                pl.semaphore_wait(barrier, devices - 1)
                for copy in part_copies:
                    copy.start()
            done = (c + 1) * chunk
            if done % group == 0 or done == length:
                pending.append((i, start, done))
                start = done
    flush()
    for copy in part_copies:
        copy.wait()

    for r in range(own_rows):
        trace, reward = rows_info[r]["trace"], rows_info[r]["reward"]
        squares = jnp.concatenate(squares_of[partner_rows + r], axis=1)
        products = jnp.concatenate(products_of[partner_rows + r], axis=1)
        for k in range(1, tensor_count):
            squares = squares + part_recv[k - 1, 2 * r : 2 * r + 1, :]
            products = products + part_recv[k - 1, 2 * r + 1 : 2 * r + 2, :]
        values = products * lax.rsqrt(squares / width + EPS_NORM)
        values_ref[r : r + 1, :] = values[0:1, :]
        pull = reward + (1.0 - trace) / trace * values
        for b in range(length // 8):
            rows = pl.ds(b * 8, 8)
            terms = reach[r, rows, :] * pull
            parts[0, 0, rows, :] = sum(
                terms[:, n * LANES : (n + 1) * LANES] for n in range(length // LANES)
            )
        ones = jnp.ones((8, LANES), jnp.bfloat16)
        adv = sum(lane_sums(ones, [piece]) for piece in split(parts[0, 0], 3)) - values / trace
        board[my_slot, r : r + 1, adv_lanes] = adv[0:1, :]
        board[my_slot, r : r + 1, offset_lanes] = jnp.broadcast_to(
            values[0:1, 0:1] + trace[0:1, 0:1] * adv[0:1, 0:1], (1, LANES)
        )

    send_all(late_lanes, late_recv_sem)

    all_blocks(early_lanes, early_recv_sem).wait()
    everyone = [
        (t * own_rows + r, pl.ds(t * seq_count, seq_count), r)
        for t in range(tensor_count)
        for r in range(own_rows)
    ]
    total = lambda x: jnp.sum(jnp.sum(x, axis=0, keepdims=True), axis=1, keepdims=True)
    count = jnp.zeros((seq_count, length), jnp.float32)
    coefs = []
    for row, slots, r in everyone:
        count = count + board[slots, r, weight_lanes]
        coef = coef_of(board[slots, r, done_lanes], row)
        coefs.append(coef)
        slope[slots, r, :] = jnp.broadcast_to(trc[row] * coef[:, 0:1], (seq_count, LANES))
    each = 1.0 / total(count)
    own_coefs = [coef_of(board[my_slot, r : r + 1, done_lanes], first_row + r) for r in range(own_rows)]
    all_blocks(late_lanes, late_recv_sem).wait()

    for row, slots, r in everyone:
        entering = jnp.full((1, LANES), boot[row], jnp.float32)
        for n in range(seq_count - 1, -1, -1):
            slot = slots.start + n
            carry[slot, r : r + 1, :] = entering
            if n:
                offset = board[slot, r : r + 1, offset_lanes]
                entering = offset + slope[slot, r : r + 1, :] * entering
    advs = []
    sums = jnp.zeros((seq_count, length), jnp.float32)
    for row, slots, r in everyone:
        entering = jnp.concatenate([carry[slots, r, :]] * (length // LANES), axis=1)
        adv = board[slots, r, adv_lanes] + coefs[row] * entering
        advs.append(adv)
        sums = sums + board[slots, r, weight_lanes] * adv
    mean = total(sums) * each

    def token_loss(ratio, weight, white):
        clipped = jnp.clip(ratio, 1.0 - CLIP, 1.0 + CLIP)
        return -weight * jnp.minimum(ratio * white, clipped * white)

    spread = jnp.zeros((seq_count, length), jnp.float32)
    losses = jnp.zeros((seq_count, length), jnp.float32)
    for row, slots, r in everyone:
        centred = advs[row] - mean
        weight = board[slots, r, weight_lanes]
        spread = spread + weight * centred * centred
        losses = losses + token_loss(board[slots, r, pl.ds(0, length)], weight, centred)
    scale = lax.rsqrt(total(spread) * each + EPS_WHITE)
    loss_ref[...] = jnp.broadcast_to(total(losses) * each * scale, (1, LANES))

    for r in range(own_rows):
        entering = jnp.concatenate([carry[my_slot, r : r + 1, :]] * (length // LANES), axis=1)
        adv = board[my_slot, r : r + 1, adv_lanes] + own_coefs[r] * entering
        white = (adv - mean) * scale
        white_ref[r : r + 1, :] = white
        token_ref[r : r + 1, :] = token_loss(rows_info[r]["ratio"], rows_info[r]["weight"], white)

    view = board.at[pl.ds(0, devices - 1)]
    pltpu.make_async_copy(view, view, send_sem).wait()


def write_out(*refs):
    half = len(refs) // 2
    for src, dst in zip(refs[:half], refs[half:]):
        dst[...] = src[:, : dst.shape[1]]


def shards(seq_count, tensor_count, *args):
    seqs_all, length, local_width = args[0].shape
    own_rows = seqs_all // tensor_count
    devices = seq_count * tensor_count
    chunk = min(length, 64)
    f32 = jnp.float32
    row = jax.ShapeDtypeStruct((own_rows, length), f32)
    dma = pltpu.SemaphoreType.DMA
    others = max(tensor_count - 1, 1)
    shapes = [row, row, row, jax.ShapeDtypeStruct((1, 1), f32)]
    near_bytes = 2 * local_width * 2 + seqs_all * length * 4
    far_bytes = (3 * own_rows + seqs_all) * length * 4
    outs = pl.pallas_call(
        functools.partial(kernel, seq_count, tensor_count, local_width * tensor_count, chunk),
        out_shape=[row, row, row, jax.ShapeDtypeStruct((1, LANES), f32)],
        in_specs=[pl.BlockSpec(memory_space=pltpu.HBM)] * 11,
        out_specs=[pl.BlockSpec(memory_space=pltpu.VMEM)] * 4,
        scratch_shapes=[
            pltpu.VMEM((seqs_all, length, local_width), jnp.bfloat16),
            pltpu.VMEM((local_width,), jnp.bfloat16),
            pltpu.VMEM((local_width,), jnp.bfloat16),
            pltpu.VMEM((seqs_all, length), f32),
            pltpu.VMEM((seqs_all, length), jnp.int32),
            pltpu.VMEM((own_rows, length), jnp.int32),
            pltpu.VMEM((own_rows, length), f32),
            pltpu.VMEM((own_rows, length), f32),
            pltpu.SMEM((seqs_all,), f32),
            pltpu.SMEM((seqs_all,), f32),
            pltpu.SMEM((seqs_all,), f32),
            pltpu.VMEM((max(near_bytes, far_bytes) // (4 * LANES), 1, LANES), f32),
            pltpu.VMEM((8, local_width), f32),
            pltpu.VMEM((2, 2, length, LANES), f32),
            pltpu.VMEM((own_rows, length, length), f32),
            pltpu.VMEM((others, 2 * own_rows, length), f32),
            pltpu.VMEM((others, 2 * own_rows, length), f32),
            pltpu.VMEM((devices, own_rows, 3 * length + 2 * LANES), f32),
            pltpu.VMEM((devices, own_rows, LANES), f32),
            pltpu.VMEM((devices, own_rows, LANES), f32),
            dma((min(seqs_all, AHEAD_ROWS) * (length // chunk),)),
            dma,
            dma,
            dma((3,)),
            dma((others,)),
            dma((others,)),
            dma,
            dma,
            dma,
        ],
        compiler_params=pltpu.CompilerParams(
            collective_id=0, has_side_effects=True, vmem_limit_bytes=24 << 20
        ),
    )(*[pltpu.with_memory_space_constraint(x, pltpu.HBM) for x in args])
    outs = pl.pallas_call(
        write_out,
        out_shape=shapes,
        in_specs=[pl.BlockSpec(memory_space=pltpu.VMEM)] * 4,
        out_specs=[pl.BlockSpec(memory_space=pltpu.VMEM)] * 4,
        compiler_params=pltpu.CompilerParams(vmem_limit_bytes=1 << 20),
    )(*outs)
    return (outs[0], outs[1], outs[2], outs[3].reshape(()))


def solution(mesh):
    in_specs = (
        P(None, "seq", "tensor"),
        P("tensor"),
        P("tensor"),
        P(None, "seq"),
        P(None, "seq"),
        P("tensor", "seq"),
        P("tensor", "seq"),
        P("tensor", "seq"),
        P(),
        P(),
        P(),
    )
    out_specs = (P("tensor", "seq"), P("tensor", "seq"), P("tensor", "seq"), P())
    body = functools.partial(shards, mesh.shape["seq"], mesh.shape["tensor"])
    return jax.shard_map(body, mesh=mesh, in_specs=in_specs, out_specs=out_specs, check_vma=False)
```

```python
import functools

import jax
import jax.numpy as jnp
from jax import lax
from jax.experimental import pallas as pl
from jax.experimental.pallas import tpu as pltpu
from jax.sharding import PartitionSpec as P

EPS_NORM = 1e-06
EPS_WHITE = 1e-08
CLIP = 0.2
LANES = 128
BLOCK = 32
UNROLLED = 64
AHEAD_ROWS = 2


def split(parts, count):
    pieces = []
    for _ in range(count):
        pieces.append(parts.astype(jnp.bfloat16))
        parts = parts - pieces[-1].astype(jnp.float32)
    return pieces


def lane_sums(ones, pieces):
    return lax.dot_general(
        ones,
        jnp.concatenate(pieces, axis=1),
        (((1,), (1,)), ((), ())),
        preferred_element_type=jnp.float32,
    )


def kernel(
    seq_count,
    tensor_count,
    width,
    chunk,
    hidden_hbm,
    gain_hbm,
    weight_hbm,
    rewards_hbm,
    flags_hbm,
    mask_hbm,
    new_hbm,
    old_hbm,
    discount_hbm,
    trace_hbm,
    boot_hbm,
    values_ref,
    white_ref,
    token_ref,
    loss_ref,
    hid,
    gain,
    wgt,
    rew,
    flg,
    msk,
    newp,
    oldp,
    disc,
    trc,
    boot,
    ruler,
    scaled,
    parts,
    reach,
    part_send,
    part_recv,
    board,
    carry,
    slope,
    hid_sem,
    near_sem,
    far_sem,
    scalar_sem,
    part_send_sem,
    part_recv_sem,
    send_sem,
    early_recv_sem,
    late_recv_sem,
):
    seqs_all, length, local_width = hid.shape
    own_rows = seqs_all // tensor_count
    devices = seq_count * tensor_count
    chunks = length // chunk
    me_seq = lax.axis_index("seq")
    me_ten = lax.axis_index("tensor")
    first_row = me_ten * own_rows
    my_slot = me_ten * seq_count + me_seq
    early_lanes = pl.ds(0, 2 * length + LANES)
    late_lanes = pl.ds(2 * length + LANES, length + LANES)
    weight_lanes = pl.ds(length, length)
    done_lanes = pl.ds(2 * length, LANES)
    adv_lanes = pl.ds(2 * length + LANES, length)
    offset_lanes = pl.ds(3 * length + LANES, LANES)

    near = [(gain_hbm, gain), (weight_hbm, wgt), (flags_hbm, flg)]
    scalars = [(discount_hbm, disc), (trace_hbm, trc), (boot_hbm, boot)]
    far = [(rewards_hbm, rew), (mask_hbm, msk), (new_hbm, newp), (old_hbm, oldp)]

    def wait_group(group, sem):
        size = sum(dst.size * dst.dtype.itemsize for _, dst in group)
        view = ruler.at[pl.ds(0, size // (4 * LANES))]
        pltpu.make_async_copy(view, view, sem).wait()

    ahead_rows = hid_sem.shape[0] // chunks

    def hid_copy(i, c):
        row = lax.rem(first_row + own_rows + i, seqs_all)
        rows = pl.ds(c * chunk, chunk)
        sem = hid_sem.at[i % ahead_rows * chunks + c]
        return pltpu.make_async_copy(hidden_hbm.at[row, rows, :], hid.at[i, rows, :], sem)

    for src, dst in near:
        pltpu.make_async_copy(src, dst, near_sem).start()
    scalar_copies = [
        pltpu.make_async_copy(src, dst, scalar_sem.at[i]) for i, (src, dst) in enumerate(scalars)
    ]
    for copy in scalar_copies[0:2]:
        copy.start()

    def prefetch(i, _):
        for c in range(chunks):
            hid_copy(i, c).start()
        return 0

    lax.fori_loop(0, ahead_rows, prefetch, 0)

    scalar_copies[2].start()
    for src, dst in far:
        pltpu.make_async_copy(src, dst, far_sem).start()

    barrier = pltpu.get_barrier_semaphore()
    bits = seq_count.bit_length() - 1
    unrolled = devices <= UNROLLED
    mirrored = unrolled and seq_count == 1 << bits
    flips = [(1 << i) * (1 - 2 * lax.rem(lax.div(me_seq, 1 << i), 2)) for i in range(bits)]

    def peer(k):
        if not mirrored:
            slot = lax.rem(my_slot + k, devices)
            return (lax.rem(slot, seq_count), lax.div(slot, seq_count))
        far, turn = divmod(devices - k, tensor_count)
        seq = me_seq
        for i in range(bits):
            if far >> i & 1:
                seq = seq + flips[i]
        return (seq, tensor_count - 1 - turn if far else lax.rem(me_ten + turn, tensor_count))

    def each_peer(act):
        if unrolled:
            for k in range(1, devices):
                act(k, 0)
        else:
            lax.fori_loop(1, devices, act, 0)

    def greet(k, _):
        pl.semaphore_signal(
            barrier, inc=1, device_id=peer(k), device_id_type=pl.DeviceIdType.MESH
        )
        return 0

    each_peer(greet)

    wait_group(near, near_sem)
    for copy in scalar_copies[0:2]:
        copy.wait()

    for j in range(local_width // LANES):
        cols = pl.ds(j * LANES, LANES)
        row = gain[cols].astype(jnp.float32) * wgt[cols].astype(jnp.float32)
        scaled[:, cols] = jnp.broadcast_to(row.reshape(1, LANES), (8, LANES))

    lane = lax.broadcasted_iota(jnp.int32, (8, length), 1).astype(jnp.float32)
    after = lax.broadcasted_iota(jnp.int32, (BLOCK, length), 1).astype(jnp.float32)
    before = lax.broadcasted_iota(jnp.int32, (BLOCK, length), 0).astype(jnp.float32)

    def coef_of(last_done, row):
        shape = last_done.shape[:-1] + (length,)
        at = lax.broadcasted_iota(jnp.int32, shape, len(shape) - 1).astype(jnp.float32)
        discount = jnp.full(shape, disc[row], jnp.float32)
        decay = discount * jnp.full(shape, trc[row], jnp.float32)
        power = jnp.exp((length - 1.0 - at) * jnp.log(decay))
        return jnp.where(at > last_done[..., 0:1], discount * power, 0.0)

    rows_info = []
    for r in range(own_rows):
        trace = jnp.full((8, length), trc[first_row + r], jnp.float32)
        decay = jnp.full((BLOCK, length), disc[first_row + r], jnp.float32) * trace[0, 0]
        log_decay = jnp.log(decay)
        flags = jnp.broadcast_to(flg[pl.ds(first_row + r, 1), :], (BLOCK, length)) > 0
        last_done = jnp.max(
            jnp.where(flags[0:8, :], lane, -1.0)[0:1, :], axis=1, keepdims=True
        )
        board[my_slot, r : r + 1, done_lanes] = jnp.broadcast_to(last_done, (1, LANES))
        rows_info.append(dict(trace=trace))
        for b in range(length // BLOCK):
            at = before + float(b * BLOCK)
            gap = after - at
            stop = jnp.where(flags & (gap >= 0.0), after, float(length))
            stop = jnp.min(stop, axis=1, keepdims=True)
            reach[r, pl.ds(b * BLOCK, BLOCK), :] = jnp.where(
                (gap >= 0.0) & (after <= stop), jnp.exp(gap * log_decay), 0.0
            )

    def add_chunk(i, c):
        for b in range(chunk // BLOCK):
            rows = pl.ds(c * chunk + b * BLOCK, BLOCK)
            squares = jnp.zeros((BLOCK // 8, 8, LANES), jnp.float32)
            products = jnp.zeros((BLOCK // 8, 8, LANES), jnp.float32)
            for j in range(local_width // LANES):
                cols = pl.ds(j * LANES, LANES)
                x = hid[i, rows, cols].astype(jnp.float32).reshape(BLOCK // 8, 8, LANES)
                squares = squares + x * x
                products = products + x * scaled[:, cols][None]
            parts[i % 2, 0, rows, :] = squares.reshape(BLOCK, LANES)
            parts[i % 2, 1, rows, :] = products.reshape(BLOCK, LANES)

    part_copies = [
        pltpu.make_async_remote_copy(
            src_ref=part_send.at[k - 1],
            dst_ref=part_recv.at[k - 1],
            send_sem=part_send_sem.at[k - 1],
            recv_sem=part_recv_sem.at[k - 1],
            device_id=(me_seq, lax.rem(me_ten + k, tensor_count)),
            device_id_type=pl.DeviceIdType.MESH,
        )
        for k in range(1, tensor_count)
    ]

    def send_all(lanes, recv_sem):
        def send(k, _):
            pltpu.make_async_remote_copy(
                src_ref=board.at[my_slot, :, lanes],
                dst_ref=board.at[my_slot, :, lanes],
                send_sem=send_sem,
                recv_sem=recv_sem,
                device_id=peer(k),
                device_id_type=pl.DeviceIdType.MESH,
            ).start()
            return 0

        each_peer(send)

    def all_blocks(lanes, sem):
        view = board.at[pl.ds(0, devices - 1), :, lanes]
        return pltpu.make_async_copy(view, view, sem)

    def publish():
        wait_group(far, far_sem)
        scalar_copies[2].wait()
        for r in range(own_rows):
            ratio = jnp.exp(newp[r : r + 1, :] - oldp[r : r + 1, :])
            weight = msk[r : r + 1, :].astype(jnp.float32)
            reward = jnp.broadcast_to(rew[pl.ds(first_row + r, 1), :], (8, length))
            rows_info[r].update(ratio=ratio, weight=weight, reward=reward)
            board[my_slot, r : r + 1, pl.ds(0, length)] = ratio
            board[my_slot, r : r + 1, weight_lanes] = weight
        send_all(early_lanes, early_recv_sem)

    squares_of = [[] for _ in range(seqs_all)]
    products_of = [[] for _ in range(seqs_all)]
    pending = []

    half = lambda axis: lax.broadcasted_iota(jnp.int32, (16, 2 * LANES), axis)
    pick = jnp.where((half(0) < 8) == (half(1) < LANES), 1.0, 0.0).astype(jnp.bfloat16)

    def flush():
        while pending:
            i, start, stop = pending.pop()
            rows = pl.ds(start, stop - start)
            squares = split(parts[i % 2, 0, rows, :], 3)
            products = split(parts[i % 2, 1, rows, :], 3)
            both = sum(lane_sums(pick, pair) for pair in zip(squares, products))
            squares_of[i].append(both[0:8, :])
            products_of[i].append(both[8:16, :])

    partner_rows = seqs_all - own_rows
    group = length
    for i in range(seqs_all):
        start = 0
        for c in range(chunks):
            hid_copy(i, c).wait()
            if i + ahead_rows < seqs_all:
                hid_copy(i + ahead_rows, c).start()
            if i > 0 and c == 1 and i <= partner_rows:
                k, r = divmod(i - 1, own_rows)
                squares = jnp.concatenate(squares_of[i - 1], axis=1)
                products = jnp.concatenate(products_of[i - 1], axis=1)
                part_send[k, 2 * r : 2 * r + 1, :] = squares[0:1, :]
                part_send[k, 2 * r + 1 : 2 * r + 2, :] = products[0:1, :]
            if i == partner_rows and c == 1:
                pl.semaphore_wait(barrier, devices - 1)
                for copy in part_copies:
                    copy.start()
            if i == partner_rows and c == 1:
                publish()
            flush()
            add_chunk(i, c)
            done = (c + 1) * chunk
            if done % group == 0 or done == length:
                pending.append((i, start, done))
                start = done
    flush()
    for copy in part_copies:
        copy.wait()

    for r in range(own_rows):
        trace, reward = rows_info[r]["trace"], rows_info[r]["reward"]
        squares = jnp.concatenate(squares_of[partner_rows + r], axis=1)
        products = jnp.concatenate(products_of[partner_rows + r], axis=1)
        for k in range(1, tensor_count):
            squares = squares + part_recv[k - 1, 2 * r : 2 * r + 1, :]
            products = products + part_recv[k - 1, 2 * r + 1 : 2 * r + 2, :]
        values = products * lax.rsqrt(squares / width + EPS_NORM)
        values_ref[r : r + 1, :] = values[0:1, :]
        pull = reward + (1.0 - trace) / trace * values
        pulled = []
        for b in range(length // 8):
            terms = reach[r, pl.ds(b * 8, 8), :] * pull
            pulled.append(sum(terms[:, n * LANES : (n + 1) * LANES] for n in range(length // LANES)))
        pulled = jnp.concatenate(pulled, axis=0)
        ones = jnp.ones((8, LANES), jnp.bfloat16)
        adv = sum(lane_sums(ones, [piece]) for piece in split(pulled, 3)) - values / trace
        board[my_slot, r : r + 1, adv_lanes] = adv[0:1, :]
        board[my_slot, r : r + 1, offset_lanes] = jnp.broadcast_to(
            values[0:1, 0:1] + trace[0:1, 0:1] * adv[0:1, 0:1], (1, LANES)
        )

    send_all(late_lanes, late_recv_sem)

    all_blocks(early_lanes, early_recv_sem).wait()
    everyone = [
        (t * own_rows + r, pl.ds(t * seq_count, seq_count), r)
        for t in range(tensor_count)
        for r in range(own_rows)
    ]
    total = lambda x: jnp.sum(jnp.sum(x, axis=0, keepdims=True), axis=1, keepdims=True)
    count = jnp.zeros((seq_count, length), jnp.float32)
    coefs = []
    for row, slots, r in everyone:
        count = count + board[slots, r, weight_lanes]
        coef = coef_of(board[slots, r, done_lanes], row)
        coefs.append(coef)
        slope[slots, r, :] = jnp.broadcast_to(trc[row] * coef[:, 0:1], (seq_count, LANES))
    each = 1.0 / total(count)
    own_coefs = [coef_of(board[my_slot, r : r + 1, done_lanes], first_row + r) for r in range(own_rows)]
    all_blocks(late_lanes, late_recv_sem).wait()

    for row, slots, r in everyone:
        entering = jnp.full((1, LANES), boot[row], jnp.float32)
        for n in range(seq_count - 1, -1, -1):
            slot = slots.start + n
            carry[slot, r : r + 1, :] = entering
            if n:
                offset = board[slot, r : r + 1, offset_lanes]
                entering = offset + slope[slot, r : r + 1, :] * entering
    advs = []
    sums = jnp.zeros((seq_count, length), jnp.float32)
    for row, slots, r in everyone:
        entering = jnp.concatenate([carry[slots, r, :]] * (length // LANES), axis=1)
        adv = board[slots, r, adv_lanes] + coefs[row] * entering
        advs.append(adv)
        sums = sums + board[slots, r, weight_lanes] * adv
    mean = total(sums) * each

    def token_loss(ratio, weight, white):
        clipped = jnp.clip(ratio, 1.0 - CLIP, 1.0 + CLIP)
        return -weight * jnp.minimum(ratio * white, clipped * white)

    spread = jnp.zeros((seq_count, length), jnp.float32)
    losses = jnp.zeros((seq_count, length), jnp.float32)
    for row, slots, r in everyone:
        centred = advs[row] - mean
        weight = board[slots, r, weight_lanes]
        spread = spread + weight * centred * centred
        losses = losses + token_loss(board[slots, r, pl.ds(0, length)], weight, centred)
    scale = lax.rsqrt(total(spread) * each + EPS_WHITE)
    loss_ref[...] = jnp.broadcast_to(total(losses) * each * scale, (1, LANES))

    for r in range(own_rows):
        entering = jnp.concatenate([carry[my_slot, r : r + 1, :]] * (length // LANES), axis=1)
        adv = board[my_slot, r : r + 1, adv_lanes] + own_coefs[r] * entering
        white = (adv - mean) * scale
        white_ref[r : r + 1, :] = white
        token_ref[r : r + 1, :] = token_loss(rows_info[r]["ratio"], rows_info[r]["weight"], white)

    view = board.at[pl.ds(0, devices - 1)]
    pltpu.make_async_copy(view, view, send_sem).wait()


def write_out(*refs):
    half = len(refs) // 2
    for src, dst in zip(refs[:half], refs[half:]):
        dst[...] = src[:, : dst.shape[1]]


def shards(seq_count, tensor_count, *args):
    seqs_all, length, local_width = args[0].shape
    own_rows = seqs_all // tensor_count
    devices = seq_count * tensor_count
    chunk = min(length, 64)
    f32 = jnp.float32
    row = jax.ShapeDtypeStruct((own_rows, length), f32)
    dma = pltpu.SemaphoreType.DMA
    others = max(tensor_count - 1, 1)
    shapes = [row, row, row, jax.ShapeDtypeStruct((1, 1), f32)]
    near_bytes = 2 * local_width * 2 + seqs_all * length * 4
    far_bytes = (3 * own_rows + seqs_all) * length * 4
    outs = pl.pallas_call(
        functools.partial(kernel, seq_count, tensor_count, local_width * tensor_count, chunk),
        out_shape=[row, row, row, jax.ShapeDtypeStruct((1, LANES), f32)],
        in_specs=[pl.BlockSpec(memory_space=pltpu.HBM)] * 11,
        out_specs=[pl.BlockSpec(memory_space=pltpu.VMEM)] * 4,
        scratch_shapes=[
            pltpu.VMEM((seqs_all, length, local_width), jnp.bfloat16),
            pltpu.VMEM((local_width,), jnp.bfloat16),
            pltpu.VMEM((local_width,), jnp.bfloat16),
            pltpu.VMEM((seqs_all, length), f32),
            pltpu.VMEM((seqs_all, length), jnp.int32),
            pltpu.VMEM((own_rows, length), jnp.int32),
            pltpu.VMEM((own_rows, length), f32),
            pltpu.VMEM((own_rows, length), f32),
            pltpu.SMEM((seqs_all,), f32),
            pltpu.SMEM((seqs_all,), f32),
            pltpu.SMEM((seqs_all,), f32),
            pltpu.VMEM((max(near_bytes, far_bytes) // (4 * LANES), 1, LANES), f32),
            pltpu.VMEM((8, local_width), f32),
            pltpu.VMEM((2, 2, length, LANES), f32),
            pltpu.VMEM((own_rows, length, length), f32),
            pltpu.VMEM((others, 2 * own_rows, length), f32),
            pltpu.VMEM((others, 2 * own_rows, length), f32),
            pltpu.VMEM((devices, own_rows, 3 * length + 2 * LANES), f32),
            pltpu.VMEM((devices, own_rows, LANES), f32),
            pltpu.VMEM((devices, own_rows, LANES), f32),
            dma((min(seqs_all, AHEAD_ROWS) * (length // chunk),)),
            dma,
            dma,
            dma((3,)),
            dma((others,)),
            dma((others,)),
            dma,
            dma,
            dma,
        ],
        compiler_params=pltpu.CompilerParams(
            collective_id=0, has_side_effects=True, vmem_limit_bytes=24 << 20
        ),
    )(*[pltpu.with_memory_space_constraint(x, pltpu.HBM) for x in args])
    outs = pl.pallas_call(
        write_out,
        out_shape=shapes,
        in_specs=[pl.BlockSpec(memory_space=pltpu.VMEM)] * 4,
        out_specs=[pl.BlockSpec(memory_space=pltpu.VMEM)] * 4,
        compiler_params=pltpu.CompilerParams(vmem_limit_bytes=1 << 20),
    )(*outs)
    return (outs[0], outs[1], outs[2], outs[3].reshape(()))


def solution(mesh):
    in_specs = (
        P(None, "seq", "tensor"),
        P("tensor"),
        P("tensor"),
        P(None, "seq"),
        P(None, "seq"),
        P("tensor", "seq"),
        P("tensor", "seq"),
        P("tensor", "seq"),
        P(),
        P(),
        P(),
    )
    out_specs = (P("tensor", "seq"), P("tensor", "seq"), P("tensor", "seq"), P())
    body = functools.partial(shards, mesh.shape["seq"], mesh.shape["tensor"])
    return jax.shard_map(body, mesh=mesh, in_specs=in_specs, out_specs=out_specs, check_vma=False)
```

```python
import functools

import jax
import jax.numpy as jnp
from jax import lax
from jax.experimental import pallas as pl
from jax.experimental.pallas import tpu as pltpu
from jax.sharding import PartitionSpec as P

EPS_NORM = 1e-06
EPS_WHITE = 1e-08
CLIP = 0.2
LANES = 128
BLOCK = 32
UNROLLED = 64
PIECES = 3
AHEAD_ROWS = 2


def split(parts, count):
    pieces = []
    for _ in range(count):
        pieces.append(parts.astype(jnp.bfloat16))
        parts = parts - pieces[-1].astype(jnp.float32)
    return pieces


def lane_sums(ones, pieces):
    return lax.dot_general(
        ones,
        jnp.concatenate(pieces, axis=1),
        (((1,), (1,)), ((), ())),
        preferred_element_type=jnp.float32,
    )


def kernel(
    seq_count,
    tensor_count,
    width,
    chunk,
    hidden_hbm,
    gain_hbm,
    weight_hbm,
    rewards_hbm,
    flags_hbm,
    mask_hbm,
    new_hbm,
    old_hbm,
    discount_hbm,
    trace_hbm,
    boot_hbm,
    values_ref,
    white_ref,
    token_ref,
    loss_ref,
    hid,
    gain,
    wgt,
    rew,
    flg,
    msk,
    newp,
    oldp,
    disc,
    trc,
    boot,
    ruler,
    scaled,
    parts,
    reach,
    part_send,
    part_recv,
    board,
    carry,
    slope,
    hid_sem,
    near_sem,
    far_sem,
    scalar_sem,
    part_send_sem,
    part_recv_sem,
    send_sem,
    early_recv_sem,
    forward_recv_sem,
    late_recv_sem,
):
    seqs_all, length, local_width = hid.shape
    own_rows = seqs_all // tensor_count
    devices = seq_count * tensor_count
    chunks = length // chunk
    me_seq = lax.axis_index("seq")
    me_ten = lax.axis_index("tensor")
    first_row = me_ten * own_rows
    my_slot = me_ten * seq_count + me_seq
    early_lanes = pl.ds(0, 2 * length + LANES)
    late_lanes = pl.ds(2 * length + LANES, length + LANES)
    weight_lanes = pl.ds(length, length)
    done_lanes = pl.ds(2 * length, LANES)
    adv_lanes = pl.ds(2 * length + LANES, length)
    offset_lanes = pl.ds(3 * length + LANES, LANES)

    near = [(gain_hbm, gain), (weight_hbm, wgt), (flags_hbm, flg)]
    scalars = [(discount_hbm, disc), (trace_hbm, trc), (boot_hbm, boot)]
    far = [(rewards_hbm, rew), (mask_hbm, msk), (new_hbm, newp), (old_hbm, oldp)]

    def wait_group(group, sem):
        size = sum(dst.size * dst.dtype.itemsize for _, dst in group)
        view = ruler.at[pl.ds(0, size // (4 * LANES))]
        pltpu.make_async_copy(view, view, sem).wait()

    ahead_rows = hid_sem.shape[0] // chunks

    def hid_copy(i, c):
        row = lax.rem(first_row + own_rows + i, seqs_all)
        rows = pl.ds(c * chunk, chunk)
        sem = hid_sem.at[i % ahead_rows * chunks + c]
        return pltpu.make_async_copy(hidden_hbm.at[row, rows, :], hid.at[i, rows, :], sem)

    for src, dst in near:
        pltpu.make_async_copy(src, dst, near_sem).start()
    scalar_copies = [
        pltpu.make_async_copy(src, dst, scalar_sem.at[i]) for i, (src, dst) in enumerate(scalars)
    ]
    for copy in scalar_copies[0:2]:
        copy.start()

    def prefetch(i, _):
        for c in range(chunks):
            hid_copy(i, c).start()
        return 0

    lax.fori_loop(0, ahead_rows, prefetch, 0)

    scalar_copies[2].start()
    for src, dst in far:
        pltpu.make_async_copy(src, dst, far_sem).start()

    barrier = pltpu.get_barrier_semaphore()
    bits = seq_count.bit_length() - 1
    unrolled = devices <= UNROLLED
    mirrored = unrolled and seq_count == 1 << bits
    flips = [(1 << i) * (1 - 2 * lax.rem(lax.div(me_seq, 1 << i), 2)) for i in range(bits)]

    def peer(k):
        if not mirrored:
            slot = lax.rem(my_slot + k, devices)
            return (lax.rem(slot, seq_count), lax.div(slot, seq_count))
        far, turn = divmod(devices - k, tensor_count)
        seq = me_seq
        for i in range(bits):
            if far >> i & 1:
                seq = seq + flips[i]
        return (seq, tensor_count - 1 - turn if far else lax.rem(me_ten + turn, tensor_count))

    def each_peer(act):
        if unrolled:
            for k in range(1, devices):
                act(k, 0)
        else:
            lax.fori_loop(1, devices, act, 0)

    def greet(k, _):
        pl.semaphore_signal(
            barrier, inc=1, device_id=peer(k), device_id_type=pl.DeviceIdType.MESH
        )
        return 0

    each_peer(greet)

    wait_group(near, near_sem)
    for copy in scalar_copies[0:2]:
        copy.wait()

    for j in range(local_width // LANES):
        cols = pl.ds(j * LANES, LANES)
        row = gain[cols].astype(jnp.float32) * wgt[cols].astype(jnp.float32)
        scaled[:, cols] = jnp.broadcast_to(row.reshape(1, LANES), (8, LANES))

    lane = lax.broadcasted_iota(jnp.int32, (8, length), 1).astype(jnp.float32)
    after = lax.broadcasted_iota(jnp.int32, (BLOCK, length), 1).astype(jnp.float32)
    before = lax.broadcasted_iota(jnp.int32, (BLOCK, length), 0).astype(jnp.float32)

    def coef_of(last_done, row):
        shape = last_done.shape[:-1] + (length,)
        at = lax.broadcasted_iota(jnp.int32, shape, len(shape) - 1).astype(jnp.float32)
        discount = jnp.full(shape, disc[row], jnp.float32)
        decay = discount * jnp.full(shape, trc[row], jnp.float32)
        power = jnp.exp((length - 1.0 - at) * jnp.log(decay))
        return jnp.where(at > last_done[..., 0:1], discount * power, 0.0)

    rows_info = []
    for r in range(own_rows):
        trace = jnp.full((8, length), trc[first_row + r], jnp.float32)
        decay = jnp.full((BLOCK, length), disc[first_row + r], jnp.float32) * trace[0, 0]
        log_decay = jnp.log(decay)
        flags = jnp.broadcast_to(flg[pl.ds(first_row + r, 1), :], (BLOCK, length)) > 0
        last_done = jnp.max(
            jnp.where(flags[0:8, :], lane, -1.0)[0:1, :], axis=1, keepdims=True
        )
        board[my_slot, r : r + 1, done_lanes] = jnp.broadcast_to(last_done, (1, LANES))
        rows_info.append(dict(trace=trace))
        for b in range(length // BLOCK):
            at = before + float(b * BLOCK)
            gap = at - after
            last = jnp.max(jnp.where(flags & (gap > 0.0), after, -1.0), axis=1, keepdims=True)
            block = jnp.where((gap >= 0.0) & (after > last), jnp.exp(gap * log_decay), 0.0)
            for n, piece in enumerate(split(block, PIECES)):
                reach[n, r, pl.ds(b * BLOCK, BLOCK), :] = piece

    def add_chunk(i, c):
        for b in range(chunk // BLOCK):
            rows = pl.ds(c * chunk + b * BLOCK, BLOCK)
            squares = jnp.zeros((BLOCK // 8, 8, LANES), jnp.float32)
            products = jnp.zeros((BLOCK // 8, 8, LANES), jnp.float32)
            for j in range(local_width // LANES):
                cols = pl.ds(j * LANES, LANES)
                x = hid[i, rows, cols].astype(jnp.float32).reshape(BLOCK // 8, 8, LANES)
                squares = squares + x * x
                products = products + x * scaled[:, cols][None]
            parts[i % 2, 0, rows, :] = squares.reshape(BLOCK, LANES)
            parts[i % 2, 1, rows, :] = products.reshape(BLOCK, LANES)

    part_copies = [
        pltpu.make_async_remote_copy(
            src_ref=part_send.at[k - 1],
            dst_ref=part_recv.at[k - 1],
            send_sem=part_send_sem.at[k - 1],
            recv_sem=part_recv_sem.at[k - 1],
            device_id=(me_seq, lax.rem(me_ten + k, tensor_count)),
            device_id_type=pl.DeviceIdType.MESH,
        )
        for k in range(1, tensor_count)
    ]

    def send_column():
        def send(k, _):
            if mirrored:
                seq = me_seq
                for i in range(bits):
                    if (seq_count - k) >> i & 1:
                        seq = seq + flips[i]
            else:
                seq = lax.rem(me_seq + k, seq_count)
            pltpu.make_async_remote_copy(
                src_ref=board.at[my_slot, :, early_lanes],
                dst_ref=board.at[my_slot, :, early_lanes],
                send_sem=send_sem,
                recv_sem=early_recv_sem,
                device_id=(seq, me_ten),
                device_id_type=pl.DeviceIdType.MESH,
            ).start()
            return 0

        if unrolled:
            for k in range(1, seq_count):
                send(k, 0)
        else:
            lax.fori_loop(1, seq_count, send, 0)

    def forward_column():
        column = board.at[pl.ds(me_ten * seq_count, seq_count), :, early_lanes]
        for k in range(1, tensor_count):
            pltpu.make_async_remote_copy(
                src_ref=column,
                dst_ref=column,
                send_sem=send_sem,
                recv_sem=forward_recv_sem,
                device_id=(me_seq, lax.rem(me_ten + k, tensor_count)),
                device_id_type=pl.DeviceIdType.MESH,
            ).start()

    def send_all(lanes, recv_sem):
        def send(k, _):
            pltpu.make_async_remote_copy(
                src_ref=board.at[my_slot, :, lanes],
                dst_ref=board.at[my_slot, :, lanes],
                send_sem=send_sem,
                recv_sem=recv_sem,
                device_id=peer(k),
                device_id_type=pl.DeviceIdType.MESH,
            ).start()
            return 0

        each_peer(send)

    def blocks(count, lanes, sem):
        view = board.at[pl.ds(0, count), :, lanes]
        return pltpu.make_async_copy(view, view, sem)

    def publish():
        wait_group(far, far_sem)
        scalar_copies[2].wait()
        for r in range(own_rows):
            ratio = jnp.exp(newp[r : r + 1, :] - oldp[r : r + 1, :])
            weight = msk[r : r + 1, :].astype(jnp.float32)
            reward = jnp.broadcast_to(rew[pl.ds(first_row + r, 1), :], (8, length))
            rows_info[r].update(ratio=ratio, weight=weight, reward=reward)
            board[my_slot, r : r + 1, pl.ds(0, length)] = ratio
            board[my_slot, r : r + 1, weight_lanes] = weight
        send_column()

    squares_of = [[] for _ in range(seqs_all)]
    products_of = [[] for _ in range(seqs_all)]
    pending = []

    half = lambda axis: lax.broadcasted_iota(jnp.int32, (16, 2 * LANES), axis)
    pick = jnp.where((half(0) < 8) == (half(1) < LANES), 1.0, 0.0).astype(jnp.bfloat16)

    def flush():
        while pending:
            i, start, stop = pending.pop()
            rows = pl.ds(start, stop - start)
            squares = split(parts[i % 2, 0, rows, :], 2)
            products = split(parts[i % 2, 1, rows, :], 3)
            both = sum(lane_sums(pick, pair) for pair in zip(squares, products))
            both = both + lane_sums(pick[:, LANES:], products[2:])
            squares_of[i].append(both[0:8, :])
            products_of[i].append(both[8:16, :])

    partner_rows = seqs_all - own_rows
    group = length
    for i in range(seqs_all):
        start = 0
        for c in range(chunks):
            hid_copy(i, c).wait()
            if i + ahead_rows < seqs_all:
                hid_copy(i + ahead_rows, c).start()
            if i > 0 and c == 1 and i <= partner_rows:
                k, r = divmod(i - 1, own_rows)
                squares = jnp.concatenate(squares_of[i - 1], axis=1)
                products = jnp.concatenate(products_of[i - 1], axis=1)
                part_send[k, 2 * r : 2 * r + 1, :] = squares[0:1, :]
                part_send[k, 2 * r + 1 : 2 * r + 2, :] = products[0:1, :]
            if i == partner_rows and c == 1:
                pl.semaphore_wait(barrier, devices - 1)
                for copy in part_copies:
                    copy.start()
            if i == partner_rows and c == 1:
                publish()
            flush()
            add_chunk(i, c)
            done = (c + 1) * chunk
            if done % group == 0 or done == length:
                pending.append((i, start, done))
                start = done
    flush()
    for copy in part_copies:
        copy.wait()

    for r in range(own_rows):
        trace, reward = rows_info[r]["trace"], rows_info[r]["reward"]
        squares = jnp.concatenate(squares_of[partner_rows + r], axis=1)
        products = jnp.concatenate(products_of[partner_rows + r], axis=1)
        for k in range(1, tensor_count):
            squares = squares + part_recv[k - 1, 2 * r : 2 * r + 1, :]
            products = products + part_recv[k - 1, 2 * r + 1 : 2 * r + 2, :]
        values = products * lax.rsqrt(squares / width + EPS_NORM)
        values_ref[r : r + 1, :] = values[0:1, :]
        pull = reward + (1.0 - trace) / trace * values
        rest, rows = pull, []
        for _ in range(PIECES):
            rows.append(rest.astype(jnp.bfloat16).astype(jnp.float32))
            rest = rest - rows[-1]
        rows = jnp.concatenate(rows + [rest], axis=0).astype(jnp.bfloat16)
        adv = -values / trace
        for n in range(PIECES):
            used = PIECES - n
            summed = lax.dot_general(
                rows[0 : 16 * pl.cdiv(used, 2), :],
                reach[n, r],
                (((1,), (0,)), ((), ())),
                preferred_element_type=jnp.float32,
            )
            for m in range(used):
                adv = adv + summed[8 * m : 8 * m + 8, :]
        board[my_slot, r : r + 1, adv_lanes] = adv[0:1, :]
        board[my_slot, r : r + 1, offset_lanes] = jnp.broadcast_to(
            values[0:1, 0:1] + trace[0:1, 0:1] * adv[0:1, 0:1], (1, LANES)
        )

    send_all(late_lanes, late_recv_sem)

    blocks(seq_count - 1, early_lanes, early_recv_sem).wait()
    forward_column()
    blocks(devices - seq_count, early_lanes, forward_recv_sem).wait()
    everyone = [
        (t * own_rows + r, pl.ds(t * seq_count, seq_count), r)
        for t in range(tensor_count)
        for r in range(own_rows)
    ]
    total = lambda x: jnp.sum(jnp.sum(x, axis=0, keepdims=True), axis=1, keepdims=True)
    count = jnp.zeros((seq_count, length), jnp.float32)
    coefs = []
    for row, slots, r in everyone:
        count = count + board[slots, r, weight_lanes]
        coef = coef_of(board[slots, r, done_lanes], row)
        coefs.append(coef)
        slope[slots, r, :] = jnp.broadcast_to(trc[row] * coef[:, 0:1], (seq_count, LANES))
    each = 1.0 / total(count)
    own_coefs = [coef_of(board[my_slot, r : r + 1, done_lanes], first_row + r) for r in range(own_rows)]
    blocks(devices - 1, late_lanes, late_recv_sem).wait()

    for row, slots, r in everyone:
        entering = jnp.full((1, LANES), boot[row], jnp.float32)
        for n in range(seq_count - 1, -1, -1):
            slot = slots.start + n
            carry[slot, r : r + 1, :] = entering
            if n:
                offset = board[slot, r : r + 1, offset_lanes]
                entering = offset + slope[slot, r : r + 1, :] * entering
    advs = []
    sums = jnp.zeros((seq_count, length), jnp.float32)
    for row, slots, r in everyone:
        entering = jnp.concatenate([carry[slots, r, :]] * (length // LANES), axis=1)
        adv = board[slots, r, adv_lanes] + coefs[row] * entering
        advs.append(adv)
        sums = sums + board[slots, r, weight_lanes] * adv
    mean = total(sums) * each

    def token_loss(ratio, weight, white):
        clipped = jnp.clip(ratio, 1.0 - CLIP, 1.0 + CLIP)
        return -weight * jnp.minimum(ratio * white, clipped * white)

    spread = jnp.zeros((seq_count, length), jnp.float32)
    losses = jnp.zeros((seq_count, length), jnp.float32)
    for row, slots, r in everyone:
        centred = advs[row] - mean
        weight = board[slots, r, weight_lanes]
        spread = spread + weight * centred * centred
        losses = losses + token_loss(board[slots, r, pl.ds(0, length)], weight, centred)
    scale = lax.rsqrt(total(spread) * each + EPS_WHITE)
    loss_ref[...] = jnp.broadcast_to(total(losses) * each * scale, (1, LANES))

    for r in range(own_rows):
        entering = jnp.concatenate([carry[my_slot, r : r + 1, :]] * (length // LANES), axis=1)
        adv = board[my_slot, r : r + 1, adv_lanes] + own_coefs[r] * entering
        white = (adv - mean) * scale
        white_ref[r : r + 1, :] = white
        token_ref[r : r + 1, :] = token_loss(rows_info[r]["ratio"], rows_info[r]["weight"], white)

    view = board.at[pl.ds(0, devices - 1)]
    pltpu.make_async_copy(view, view, send_sem).wait()


def write_out(*refs):
    half = len(refs) // 2
    for src, dst in zip(refs[:half], refs[half:]):
        dst[...] = src[:, : dst.shape[1]]


def shards(seq_count, tensor_count, *args):
    seqs_all, length, local_width = args[0].shape
    own_rows = seqs_all // tensor_count
    devices = seq_count * tensor_count
    chunk = min(length, 64)
    f32 = jnp.float32
    row = jax.ShapeDtypeStruct((own_rows, length), f32)
    dma = pltpu.SemaphoreType.DMA
    others = max(tensor_count - 1, 1)
    shapes = [row, row, row, jax.ShapeDtypeStruct((1, 1), f32)]
    near_bytes = 2 * local_width * 2 + seqs_all * length * 4
    far_bytes = (3 * own_rows + seqs_all) * length * 4
    outs = pl.pallas_call(
        functools.partial(kernel, seq_count, tensor_count, local_width * tensor_count, chunk),
        out_shape=[row, row, row, jax.ShapeDtypeStruct((1, LANES), f32)],
        in_specs=[pl.BlockSpec(memory_space=pltpu.HBM)] * 11,
        out_specs=[pl.BlockSpec(memory_space=pltpu.VMEM)] * 4,
        scratch_shapes=[
            pltpu.VMEM((seqs_all, length, local_width), jnp.bfloat16),
            pltpu.VMEM((local_width,), jnp.bfloat16),
            pltpu.VMEM((local_width,), jnp.bfloat16),
            pltpu.VMEM((seqs_all, length), f32),
            pltpu.VMEM((seqs_all, length), jnp.int32),
            pltpu.VMEM((own_rows, length), jnp.int32),
            pltpu.VMEM((own_rows, length), f32),
            pltpu.VMEM((own_rows, length), f32),
            pltpu.SMEM((seqs_all,), f32),
            pltpu.SMEM((seqs_all,), f32),
            pltpu.SMEM((seqs_all,), f32),
            pltpu.VMEM((max(near_bytes, far_bytes) // (4 * LANES), 1, LANES), f32),
            pltpu.VMEM((8, local_width), f32),
            pltpu.VMEM((2, 2, length, LANES), f32),
            pltpu.VMEM((PIECES, own_rows, length, length), jnp.bfloat16),
            pltpu.VMEM((others, 2 * own_rows, length), f32),
            pltpu.VMEM((others, 2 * own_rows, length), f32),
            pltpu.VMEM((devices, own_rows, 3 * length + 2 * LANES), f32),
            pltpu.VMEM((devices, own_rows, LANES), f32),
            pltpu.VMEM((devices, own_rows, LANES), f32),
            dma((min(seqs_all, AHEAD_ROWS) * (length // chunk),)),
            dma,
            dma,
            dma((3,)),
            dma((others,)),
            dma((others,)),
            dma,
            dma,
            dma,
            dma,
        ],
        compiler_params=pltpu.CompilerParams(
            collective_id=0, has_side_effects=True, vmem_limit_bytes=24 << 20
        ),
    )(*[pltpu.with_memory_space_constraint(x, pltpu.HBM) for x in args])
    outs = pl.pallas_call(
        write_out,
        out_shape=shapes,
        in_specs=[pl.BlockSpec(memory_space=pltpu.VMEM)] * 4,
        out_specs=[pl.BlockSpec(memory_space=pltpu.VMEM)] * 4,
        compiler_params=pltpu.CompilerParams(vmem_limit_bytes=1 << 20),
    )(*outs)
    return (outs[0], outs[1], outs[2], outs[3].reshape(()))


def solution(mesh):
    in_specs = (
        P(None, "seq", "tensor"),
        P("tensor"),
        P("tensor"),
        P(None, "seq"),
        P(None, "seq"),
        P("tensor", "seq"),
        P("tensor", "seq"),
        P("tensor", "seq"),
        P(),
        P(),
        P(),
    )
    out_specs = (P("tensor", "seq"), P("tensor", "seq"), P("tensor", "seq"), P())
    body = functools.partial(shards, mesh.shape["seq"], mesh.shape["tensor"])
    return jax.shard_map(body, mesh=mesh, in_specs=in_specs, out_specs=out_specs, check_vma=False)
```

```python
import functools

import jax
import jax.numpy as jnp
from jax import lax
from jax.experimental import pallas as pl
from jax.experimental.pallas import tpu as pltpu
from jax.sharding import PartitionSpec as P

EPS_NORM = 1e-06
EPS_WHITE = 1e-08
CLIP = 0.2
LANES = 128
BLOCK = 32
UNROLLED = 64
PIECES = 3
AHEAD_ROWS = 2


def split(parts, count):
    pieces = []
    for _ in range(count):
        pieces.append(parts.astype(jnp.bfloat16))
        parts = parts - pieces[-1].astype(jnp.float32)
    return pieces


def lane_sums(ones, pieces):
    return lax.dot_general(
        ones,
        jnp.concatenate(pieces, axis=1),
        (((1,), (1,)), ((), ())),
        preferred_element_type=jnp.float32,
    )


def kernel(
    seq_count,
    tensor_count,
    width,
    chunk,
    hidden_hbm,
    gain_hbm,
    weight_hbm,
    rewards_hbm,
    flags_hbm,
    mask_hbm,
    new_hbm,
    old_hbm,
    discount_hbm,
    trace_hbm,
    boot_hbm,
    values_ref,
    white_ref,
    token_ref,
    loss_ref,
    hid,
    gain,
    wgt,
    rew,
    flg,
    msk,
    newp,
    oldp,
    disc,
    trc,
    boot,
    ruler,
    scaled,
    parts,
    reach,
    part_send,
    part_recv,
    board,
    carry,
    slope,
    hid_sem,
    near_sem,
    far_sem,
    scalar_sem,
    part_send_sem,
    part_recv_sem,
    send_sem,
    early_recv_sem,
    forward_recv_sem,
    late_recv_sem,
):
    seqs_all, length, local_width = hid.shape
    own_rows = seqs_all // tensor_count
    devices = seq_count * tensor_count
    chunks = length // chunk
    me_seq = lax.axis_index("seq")
    me_ten = lax.axis_index("tensor")
    first_row = me_ten * own_rows
    my_slot = me_ten * seq_count + me_seq
    early_lanes = pl.ds(0, 2 * length + LANES)
    late_lanes = pl.ds(2 * length + LANES, length + LANES)
    weight_lanes = pl.ds(length, length)
    done_lanes = pl.ds(2 * length, LANES)
    adv_lanes = pl.ds(2 * length + LANES, length)
    offset_lanes = pl.ds(3 * length + LANES, LANES)

    near = [(gain_hbm, gain), (weight_hbm, wgt), (flags_hbm, flg)]
    scalars = [(discount_hbm, disc), (trace_hbm, trc), (boot_hbm, boot)]
    far = [(rewards_hbm, rew), (mask_hbm, msk), (new_hbm, newp), (old_hbm, oldp)]

    def wait_group(group, sem):
        size = sum(dst.size * dst.dtype.itemsize for _, dst in group)
        view = ruler.at[pl.ds(0, size // (4 * LANES))]
        pltpu.make_async_copy(view, view, sem).wait()

    ahead_rows = hid_sem.shape[0] // chunks

    def hid_copy(i, c):
        row = lax.rem(first_row + own_rows + i, seqs_all)
        rows = pl.ds(c * chunk, chunk)
        sem = hid_sem.at[i % ahead_rows * chunks + c]
        return pltpu.make_async_copy(hidden_hbm.at[row, rows, :], hid.at[i, rows, :], sem)

    for src, dst in near:
        pltpu.make_async_copy(src, dst, near_sem).start()
    scalar_copies = [
        pltpu.make_async_copy(src, dst, scalar_sem.at[i]) for i, (src, dst) in enumerate(scalars)
    ]
    for copy in scalar_copies[0:2]:
        copy.start()

    def prefetch(i, _):
        for c in range(chunks):
            hid_copy(i, c).start()
        return 0

    lax.fori_loop(0, ahead_rows, prefetch, 0)

    scalar_copies[2].start()
    for src, dst in far:
        pltpu.make_async_copy(src, dst, far_sem).start()

    barrier = pltpu.get_barrier_semaphore()
    bits = seq_count.bit_length() - 1
    unrolled = devices <= UNROLLED
    mirrored = unrolled and seq_count == 1 << bits
    flips = [(1 << i) * (1 - 2 * lax.rem(lax.div(me_seq, 1 << i), 2)) for i in range(bits)]

    def peer(k):
        if not mirrored:
            slot = lax.rem(my_slot + k, devices)
            return (lax.rem(slot, seq_count), lax.div(slot, seq_count))
        far, turn = divmod(devices - k, tensor_count)
        seq = me_seq
        for i in range(bits):
            if far >> i & 1:
                seq = seq + flips[i]
        return (seq, tensor_count - 1 - turn if far else lax.rem(me_ten + turn, tensor_count))

    def each_peer(act):
        if unrolled:
            for k in range(1, devices):
                act(k, 0)
        else:
            lax.fori_loop(1, devices, act, 0)

    def greet(k, _):
        pl.semaphore_signal(
            barrier, inc=1, device_id=peer(k), device_id_type=pl.DeviceIdType.MESH
        )
        return 0

    each_peer(greet)

    wait_group(near, near_sem)
    for copy in scalar_copies[0:2]:
        copy.wait()

    for j in range(local_width // LANES):
        cols = pl.ds(j * LANES, LANES)
        row = gain[cols].astype(jnp.float32) * wgt[cols].astype(jnp.float32)
        scaled[:, cols] = jnp.broadcast_to(row.reshape(1, LANES), (8, LANES))

    lane = lax.broadcasted_iota(jnp.int32, (8, length), 1).astype(jnp.float32)
    after = lax.broadcasted_iota(jnp.int32, (BLOCK, length), 1).astype(jnp.float32)
    before = lax.broadcasted_iota(jnp.int32, (BLOCK, length), 0).astype(jnp.float32)

    def coef_of(last_done, row):
        shape = last_done.shape[:-1] + (length,)
        at = lax.broadcasted_iota(jnp.int32, shape, len(shape) - 1).astype(jnp.float32)
        discount = jnp.full(shape, disc[row], jnp.float32)
        decay = discount * jnp.full(shape, trc[row], jnp.float32)
        power = jnp.exp((length - 1.0 - at) * jnp.log(decay))
        return jnp.where(at > last_done[..., 0:1], discount * power, 0.0)

    rows_info = []
    for r in range(own_rows):
        trace = jnp.full((8, length), trc[first_row + r], jnp.float32)
        decay = jnp.full((BLOCK, length), disc[first_row + r], jnp.float32) * trace[0, 0]
        log_decay = jnp.log(decay)
        flags = jnp.broadcast_to(flg[pl.ds(first_row + r, 1), :], (BLOCK, length)) > 0
        last_done = jnp.max(
            jnp.where(flags[0:8, :], lane, -1.0)[0:1, :], axis=1, keepdims=True
        )
        board[my_slot, r : r + 1, done_lanes] = jnp.broadcast_to(last_done, (1, LANES))
        rows_info.append(dict(trace=trace))
        for b in range(length // BLOCK):
            at = before + float(b * BLOCK)
            gap = at - after
            last = jnp.max(jnp.where(flags & (gap > 0.0), after, -1.0), axis=1, keepdims=True)
            block = jnp.where((gap >= 0.0) & (after > last), jnp.exp(gap * log_decay), 0.0)
            for n, piece in enumerate(split(block, PIECES)):
                reach[n, r, pl.ds(b * BLOCK, BLOCK), :] = piece

    def add_chunk(i, c):
        for b in range(chunk // BLOCK):
            rows = pl.ds(c * chunk + b * BLOCK, BLOCK)
            squares = jnp.zeros((BLOCK // 8, 8, LANES), jnp.float32)
            products = jnp.zeros((BLOCK // 8, 8, LANES), jnp.float32)
            for j in range(local_width // LANES):
                cols = pl.ds(j * LANES, LANES)
                x = hid[i, rows, cols].astype(jnp.float32).reshape(BLOCK // 8, 8, LANES)
                squares = squares + x * x
                products = products + x * scaled[:, cols][None]
            parts[i % 2, 0, rows, :] = squares.reshape(BLOCK, LANES)
            parts[i % 2, 1, rows, :] = products.reshape(BLOCK, LANES)

    part_copies = [
        pltpu.make_async_remote_copy(
            src_ref=part_send.at[k - 1],
            dst_ref=part_recv.at[k - 1],
            send_sem=part_send_sem.at[k - 1],
            recv_sem=part_recv_sem.at[k - 1],
            device_id=(me_seq, lax.rem(me_ten + k, tensor_count)),
            device_id_type=pl.DeviceIdType.MESH,
        )
        for k in range(1, tensor_count)
    ]

    def send_column():
        def send(k, _):
            if mirrored:
                seq = me_seq
                for i in range(bits):
                    if (seq_count - k) >> i & 1:
                        seq = seq + flips[i]
            else:
                seq = lax.rem(me_seq + k, seq_count)
            pltpu.make_async_remote_copy(
                src_ref=board.at[my_slot, :, early_lanes],
                dst_ref=board.at[my_slot, :, early_lanes],
                send_sem=send_sem,
                recv_sem=early_recv_sem,
                device_id=(seq, me_ten),
                device_id_type=pl.DeviceIdType.MESH,
            ).start()
            return 0

        if unrolled:
            for k in range(1, seq_count):
                send(k, 0)
        else:
            lax.fori_loop(1, seq_count, send, 0)

    def forward_column():
        column = board.at[pl.ds(me_ten * seq_count, seq_count), :, early_lanes]
        for k in range(1, tensor_count):
            pltpu.make_async_remote_copy(
                src_ref=column,
                dst_ref=column,
                send_sem=send_sem,
                recv_sem=forward_recv_sem,
                device_id=(me_seq, lax.rem(me_ten + k, tensor_count)),
                device_id_type=pl.DeviceIdType.MESH,
            ).start()

    def send_all(lanes, recv_sem):
        def send(k, _):
            pltpu.make_async_remote_copy(
                src_ref=board.at[my_slot, :, lanes],
                dst_ref=board.at[my_slot, :, lanes],
                send_sem=send_sem,
                recv_sem=recv_sem,
                device_id=peer(k),
                device_id_type=pl.DeviceIdType.MESH,
            ).start()
            return 0

        each_peer(send)

    def blocks(count, lanes, sem):
        view = board.at[pl.ds(0, count), :, lanes]
        return pltpu.make_async_copy(view, view, sem)

    def publish():
        wait_group(far, far_sem)
        scalar_copies[2].wait()
        for r in range(own_rows):
            ratio = jnp.exp(newp[r : r + 1, :] - oldp[r : r + 1, :])
            weight = msk[r : r + 1, :].astype(jnp.float32)
            reward = jnp.broadcast_to(rew[pl.ds(first_row + r, 1), :], (8, length))
            rows_info[r].update(ratio=ratio, weight=weight, reward=reward)
            board[my_slot, r : r + 1, pl.ds(0, length)] = ratio
            board[my_slot, r : r + 1, weight_lanes] = weight
        send_column()

    squares_of = [[] for _ in range(seqs_all)]
    products_of = [[] for _ in range(seqs_all)]
    pending = []

    half = lambda axis: lax.broadcasted_iota(jnp.int32, (16, 2 * LANES), axis)
    pick = jnp.where((half(0) < 8) == (half(1) < LANES), 1.0, 0.0).astype(jnp.bfloat16)

    def flush():
        while pending:
            i, start, stop = pending.pop(0)
            rows = pl.ds(start, stop - start)
            squares = split(parts[i % 2, 0, rows, :], 2)
            products = split(parts[i % 2, 1, rows, :], 3)
            both = sum(lane_sums(pick, pair) for pair in zip(squares, products))
            both = both + lane_sums(pick[:, LANES:], products[2:])
            squares_of[i].append(both[0:8, :])
            products_of[i].append(both[8:16, :])

    partner_rows = seqs_all - own_rows
    for i in range(seqs_all):
        start = 0
        for c in range(chunks):
            hid_copy(i, c).wait()
            if i + ahead_rows < seqs_all:
                hid_copy(i + ahead_rows, c).start()
            if i > 0 and c == 1 and i <= partner_rows:
                k, r = divmod(i - 1, own_rows)
                squares = jnp.concatenate(squares_of[i - 1], axis=1)
                products = jnp.concatenate(products_of[i - 1], axis=1)
                part_send[k, 2 * r : 2 * r + 1, :] = squares[0:1, :]
                part_send[k, 2 * r + 1 : 2 * r + 2, :] = products[0:1, :]
            if i == partner_rows and c == 1:
                pl.semaphore_wait(barrier, devices - 1)
                for copy in part_copies:
                    copy.start()
            if i == partner_rows and c == 1:
                publish()
            if i < partner_rows or c in (0, chunks - 1):
                flush()
            add_chunk(i, c)
            done = (c + 1) * chunk
            if done == length or i >= partner_rows and done % LANES == 0:
                pending.append((i, start, done))
                start = done
    flush()
    for copy in part_copies:
        copy.wait()

    for r in range(own_rows):
        trace, reward = rows_info[r]["trace"], rows_info[r]["reward"]
        squares = jnp.concatenate(squares_of[partner_rows + r], axis=1)
        products = jnp.concatenate(products_of[partner_rows + r], axis=1)
        for k in range(1, tensor_count):
            squares = squares + part_recv[k - 1, 2 * r : 2 * r + 1, :]
            products = products + part_recv[k - 1, 2 * r + 1 : 2 * r + 2, :]
        values = products * lax.rsqrt(squares / width + EPS_NORM)
        values_ref[r : r + 1, :] = values[0:1, :]
        pull = reward + (1.0 - trace) / trace * values
        rest, rows = pull, []
        for _ in range(PIECES):
            rows.append(rest.astype(jnp.bfloat16).astype(jnp.float32))
            rest = rest - rows[-1]
        rows = jnp.concatenate(rows + [rest], axis=0).astype(jnp.bfloat16)
        adv = -values / trace
        for n in range(PIECES):
            used = PIECES - n
            summed = lax.dot_general(
                rows[0 : 16 * pl.cdiv(used, 2), :],
                reach[n, r],
                (((1,), (0,)), ((), ())),
                preferred_element_type=jnp.float32,
            )
            for m in range(used):
                adv = adv + summed[8 * m : 8 * m + 8, :]
        board[my_slot, r : r + 1, adv_lanes] = adv[0:1, :]
        board[my_slot, r : r + 1, offset_lanes] = jnp.broadcast_to(
            values[0:1, 0:1] + trace[0:1, 0:1] * adv[0:1, 0:1], (1, LANES)
        )

    send_all(late_lanes, late_recv_sem)

    blocks(seq_count - 1, early_lanes, early_recv_sem).wait()
    forward_column()
    blocks(devices - seq_count, early_lanes, forward_recv_sem).wait()
    everyone = [
        (t * own_rows + r, pl.ds(t * seq_count, seq_count), r)
        for t in range(tensor_count)
        for r in range(own_rows)
    ]
    total = lambda x: jnp.sum(jnp.sum(x, axis=0, keepdims=True), axis=1, keepdims=True)
    def gather(slots, r, start):
        return jnp.concatenate(
            [board[slots, r, pl.ds(start + n, LANES)] for n in range(0, length, LANES)], axis=1
        )

    count = jnp.zeros((seq_count, length), jnp.float32)
    coefs, chains = [], []
    place = lax.broadcasted_iota(jnp.int32, (seq_count, LANES), 0)
    for row, slots, r in everyone:
        count = count + gather(slots, r, length)
        coef = coef_of(board[slots, r, done_lanes], row)
        coefs.append(coef)
        slope[slots, r, :] = jnp.broadcast_to(trc[row] * coef[:, 0:1], (seq_count, LANES))
        chain = [jnp.where(place == 0, 1.0, 0.0)]
        for n in range(1, seq_count):
            step = slope[slots.start + n, r : r + 1, :]
            chain.append(jnp.where(place == n, 1.0, chain[-1] * step))
        chains.append(chain)
    each = 1.0 / total(count)
    own_coefs = [coef_of(board[my_slot, r : r + 1, done_lanes], first_row + r) for r in range(own_rows)]
    blocks(devices - 1, late_lanes, late_recv_sem).wait()

    advs = []
    sums = jnp.zeros((seq_count, length), jnp.float32)
    for row, slots, r in everyone:
        terms = [boot[row] * chains[row][-1]]
        for n in range(1, seq_count):
            offset = board[slots.start + n, r : r + 1, offset_lanes]
            terms.append(chains[row][n - 1] * offset)
        while len(terms) > 1:
            terms = [sum(terms[n : n + 2]) for n in range(0, len(terms), 2)]
        carry[slots, r, :] = terms[0]
        entering = jnp.concatenate(terms * (length // LANES), axis=1)
        adv = gather(slots, r, adv_lanes.start) + coefs[row] * entering
        advs.append(adv)
        sums = sums + gather(slots, r, length) * adv
    mean = total(sums) * each

    def token_loss(ratio, weight, white):
        clipped = jnp.clip(ratio, 1.0 - CLIP, 1.0 + CLIP)
        return -weight * jnp.minimum(ratio * white, clipped * white)

    spread = jnp.zeros((seq_count, length), jnp.float32)
    losses = jnp.zeros((seq_count, length), jnp.float32)
    for row, slots, r in everyone:
        centred = advs[row] - mean
        weight = gather(slots, r, length)
        spread = spread + weight * centred * centred
        losses = losses + token_loss(gather(slots, r, 0), weight, centred)
    scale = lax.rsqrt(total(spread) * each + EPS_WHITE)
    loss_ref[...] = jnp.broadcast_to(total(losses) * each * scale, (1, LANES))

    for r in range(own_rows):
        entering = jnp.concatenate([carry[my_slot, r : r + 1, :]] * (length // LANES), axis=1)
        adv = board[my_slot, r : r + 1, adv_lanes] + own_coefs[r] * entering
        white = (adv - mean) * scale
        white_ref[r : r + 1, :] = white
        token_ref[r : r + 1, :] = token_loss(rows_info[r]["ratio"], rows_info[r]["weight"], white)

    view = board.at[pl.ds(0, devices - 1)]
    pltpu.make_async_copy(view, view, send_sem).wait()


def write_out(*refs):
    half = len(refs) // 2
    for src, dst in zip(refs[:half], refs[half:]):
        dst[...] = src[:, : dst.shape[1]]


def shards(seq_count, tensor_count, *args):
    seqs_all, length, local_width = args[0].shape
    own_rows = seqs_all // tensor_count
    devices = seq_count * tensor_count
    chunk = min(length, 64)
    f32 = jnp.float32
    row = jax.ShapeDtypeStruct((own_rows, length), f32)
    dma = pltpu.SemaphoreType.DMA
    others = max(tensor_count - 1, 1)
    shapes = [row, row, row, jax.ShapeDtypeStruct((1, 1), f32)]
    near_bytes = 2 * local_width * 2 + seqs_all * length * 4
    far_bytes = (3 * own_rows + seqs_all) * length * 4
    outs = pl.pallas_call(
        functools.partial(kernel, seq_count, tensor_count, local_width * tensor_count, chunk),
        out_shape=[row, row, row, jax.ShapeDtypeStruct((1, LANES), f32)],
        in_specs=[pl.BlockSpec(memory_space=pltpu.HBM)] * 11,
        out_specs=[pl.BlockSpec(memory_space=pltpu.VMEM)] * 4,
        scratch_shapes=[
            pltpu.VMEM((seqs_all, length, local_width), jnp.bfloat16),
            pltpu.VMEM((local_width,), jnp.bfloat16),
            pltpu.VMEM((local_width,), jnp.bfloat16),
            pltpu.VMEM((seqs_all, length), f32),
            pltpu.VMEM((seqs_all, length), jnp.int32),
            pltpu.VMEM((own_rows, length), jnp.int32),
            pltpu.VMEM((own_rows, length), f32),
            pltpu.VMEM((own_rows, length), f32),
            pltpu.SMEM((seqs_all,), f32),
            pltpu.SMEM((seqs_all,), f32),
            pltpu.SMEM((seqs_all,), f32),
            pltpu.VMEM((max(near_bytes, far_bytes) // (4 * LANES), 1, LANES), f32),
            pltpu.VMEM((8, local_width), f32),
            pltpu.VMEM((2, 2, length, LANES), f32),
            pltpu.VMEM((PIECES, own_rows, length, length), jnp.bfloat16),
            pltpu.VMEM((others, 2 * own_rows, length), f32),
            pltpu.VMEM((others, 2 * own_rows, length), f32),
            pltpu.VMEM((devices, own_rows, 3 * length + 2 * LANES), f32),
            pltpu.VMEM((devices, own_rows, LANES), f32),
            pltpu.VMEM((devices, own_rows, LANES), f32),
            dma((min(seqs_all, AHEAD_ROWS) * (length // chunk),)),
            dma,
            dma,
            dma((3,)),
            dma((others,)),
            dma((others,)),
            dma,
            dma,
            dma,
            dma,
        ],
        compiler_params=pltpu.CompilerParams(
            collective_id=0, has_side_effects=True, vmem_limit_bytes=24 << 20
        ),
    )(*[pltpu.with_memory_space_constraint(x, pltpu.HBM) for x in args])
    outs = pl.pallas_call(
        write_out,
        out_shape=shapes,
        in_specs=[pl.BlockSpec(memory_space=pltpu.VMEM)] * 4,
        out_specs=[pl.BlockSpec(memory_space=pltpu.VMEM)] * 4,
        compiler_params=pltpu.CompilerParams(vmem_limit_bytes=1 << 20),
    )(*outs)
    return (outs[0], outs[1], outs[2], outs[3].reshape(()))


def solution(mesh):
    in_specs = (
        P(None, "seq", "tensor"),
        P("tensor"),
        P("tensor"),
        P(None, "seq"),
        P(None, "seq"),
        P("tensor", "seq"),
        P("tensor", "seq"),
        P("tensor", "seq"),
        P(),
        P(),
        P(),
    )
    out_specs = (P("tensor", "seq"), P("tensor", "seq"), P("tensor", "seq"), P())
    body = functools.partial(shards, mesh.shape["seq"], mesh.shape["tensor"])
    return jax.shard_map(body, mesh=mesh, in_specs=in_specs, out_specs=out_specs, check_vma=False)
```

```python
import functools

import jax
import jax.numpy as jnp
from jax import lax
from jax.experimental import pallas as pl
from jax.experimental.pallas import tpu as pltpu
from jax.sharding import PartitionSpec as P

EPS_NORM = 1e-06
EPS_WHITE = 1e-08
CLIP = 0.2
LANES = 128
BLOCK = 32
UNROLLED = 64
PIECES = 3
AHEAD_ROWS = 2


def split(parts, count):
    pieces = []
    for _ in range(count):
        pieces.append(parts.astype(jnp.bfloat16))
        parts = parts - pieces[-1].astype(jnp.float32)
    return pieces


def lane_sums(ones, pieces):
    return lax.dot_general(
        ones,
        jnp.concatenate(pieces, axis=1),
        (((1,), (1,)), ((), ())),
        preferred_element_type=jnp.float32,
    )


def kernel(
    seq_count,
    tensor_count,
    width,
    chunk,
    hidden_hbm,
    gain_hbm,
    weight_hbm,
    rewards_hbm,
    flags_hbm,
    mask_hbm,
    new_hbm,
    old_hbm,
    discount_hbm,
    trace_hbm,
    boot_hbm,
    values_ref,
    white_ref,
    token_ref,
    loss_ref,
    hid,
    gain,
    wgt,
    rew,
    flg,
    msk,
    newp,
    oldp,
    disc,
    trc,
    boot,
    ruler,
    scaled,
    parts,
    reach,
    part_send,
    part_recv,
    board,
    carry,
    slope,
    hid_sem,
    near_sem,
    far_sem,
    scalar_sem,
    part_recv_sem,
    send_sem,
    early_recv_sem,
    forward_recv_sem,
    late_recv_sem,
):
    seqs_all, length, local_width = hid.shape
    own_rows = seqs_all // tensor_count
    devices = seq_count * tensor_count
    chunks = length // chunk
    me_seq = lax.axis_index("seq")
    me_ten = lax.axis_index("tensor")
    first_row = me_ten * own_rows
    my_slot = me_ten * seq_count + me_seq
    early_lanes = pl.ds(0, 2 * length + LANES)
    late_lanes = pl.ds(2 * length + LANES, length + LANES)
    weight_lanes = pl.ds(length, length)
    done_lanes = pl.ds(2 * length, LANES)
    adv_lanes = pl.ds(2 * length + LANES, length)
    offset_lanes = pl.ds(3 * length + LANES, LANES)

    near = [(gain_hbm, gain), (weight_hbm, wgt), (flags_hbm, flg)]
    scalars = [(discount_hbm, disc), (trace_hbm, trc), (boot_hbm, boot)]
    far = [(rewards_hbm, rew), (mask_hbm, msk), (new_hbm, newp), (old_hbm, oldp)]

    def wait_group(group, sem):
        size = sum(dst.size * dst.dtype.itemsize for _, dst in group)
        view = ruler.at[pl.ds(0, size // (4 * LANES))]
        pltpu.make_async_copy(view, view, sem).wait()

    ahead_rows = hid_sem.shape[0] // chunks

    def hid_copy(i, c):
        row = lax.rem(first_row + own_rows + i, seqs_all)
        rows = pl.ds(c * chunk, chunk)
        sem = hid_sem.at[i % ahead_rows * chunks + c]
        return pltpu.make_async_copy(hidden_hbm.at[row, rows, :], hid.at[i, rows, :], sem)

    for src, dst in near:
        pltpu.make_async_copy(src, dst, near_sem).start()
    scalar_copies = [
        pltpu.make_async_copy(src, dst, scalar_sem.at[i % 2]) for i, (src, dst) in enumerate(scalars)
    ]
    for copy in scalar_copies[0:2]:
        copy.start()

    def prefetch(i, _):
        for c in range(chunks):
            hid_copy(i, c).start()
        return 0

    lax.fori_loop(0, ahead_rows, prefetch, 0)

    for src, dst in far:
        pltpu.make_async_copy(src, dst, far_sem).start()

    barrier = pltpu.get_barrier_semaphore()
    bits = seq_count.bit_length() - 1
    unrolled = devices <= UNROLLED
    mirrored = unrolled and seq_count == 1 << bits
    flips = [(1 << i) * (1 - 2 * lax.rem(lax.div(me_seq, 1 << i), 2)) for i in range(bits)]

    def peer(k):
        if not mirrored:
            slot = lax.rem(my_slot + k, devices)
            return (lax.rem(slot, seq_count), lax.div(slot, seq_count))
        far, turn = divmod(devices - k, tensor_count)
        seq = me_seq
        for i in range(bits):
            if far >> i & 1:
                seq = seq + flips[i]
        return (seq, tensor_count - 1 - turn if far else lax.rem(me_ten + turn, tensor_count))

    def each_peer(act):
        if unrolled:
            for k in range(1, devices):
                act(k, 0)
        else:
            lax.fori_loop(1, devices, act, 0)

    def greet(k, _):
        pl.semaphore_signal(
            barrier, inc=1, device_id=peer(k), device_id_type=pl.DeviceIdType.MESH
        )
        return 0

    each_peer(greet)

    wait_group(near, near_sem)
    for copy in scalar_copies[0:2]:
        copy.wait()
    scalar_copies[2].start()

    for j in range(local_width // LANES):
        cols = pl.ds(j * LANES, LANES)
        row = gain[cols].astype(jnp.float32) * wgt[cols].astype(jnp.float32)
        scaled[:, cols] = jnp.broadcast_to(row.reshape(1, LANES), (8, LANES))

    lane = lax.broadcasted_iota(jnp.int32, (8, length), 1).astype(jnp.float32)
    after = lax.broadcasted_iota(jnp.int32, (BLOCK, length), 1).astype(jnp.float32)
    before = lax.broadcasted_iota(jnp.int32, (BLOCK, length), 0).astype(jnp.float32)

    def coef_of(last_done, row):
        shape = last_done.shape[:-1] + (length,)
        at = lax.broadcasted_iota(jnp.int32, shape, len(shape) - 1).astype(jnp.float32)
        discount = jnp.full(shape, disc[row], jnp.float32)
        decay = discount * jnp.full(shape, trc[row], jnp.float32)
        power = jnp.exp((length - 1.0 - at) * jnp.log(decay))
        return jnp.where(at > last_done[..., 0:1], discount * power, 0.0)

    rows_info = []
    for r in range(own_rows):
        trace = jnp.full((8, length), trc[first_row + r], jnp.float32)
        decay = jnp.full((BLOCK, length), disc[first_row + r], jnp.float32) * trace[0, 0]
        log_decay = jnp.log(decay)
        flags = jnp.broadcast_to(flg[pl.ds(first_row + r, 1), :], (BLOCK, length)) > 0
        last_done = jnp.max(
            jnp.where(flags[0:8, :], lane, -1.0)[0:1, :], axis=1, keepdims=True
        )
        board[my_slot, r : r + 1, done_lanes] = jnp.broadcast_to(last_done, (1, LANES))
        rows_info.append(dict(trace=trace))
        for b in range(length // BLOCK):
            at = before + float(b * BLOCK)
            gap = at - after
            last = jnp.max(jnp.where(flags & (gap > 0.0), after, -1.0), axis=1, keepdims=True)
            block = jnp.where((gap >= 0.0) & (after > last), jnp.exp(gap * log_decay), 0.0)
            for n, piece in enumerate(split(block, PIECES)):
                reach[n, r, pl.ds(b * BLOCK, BLOCK), :] = piece

    def add_chunk(i, c):
        for b in range(chunk // BLOCK):
            rows = pl.ds(c * chunk + b * BLOCK, BLOCK)
            squares = jnp.zeros((BLOCK // 8, 8, LANES), jnp.float32)
            products = jnp.zeros((BLOCK // 8, 8, LANES), jnp.float32)
            for j in range(local_width // LANES):
                cols = pl.ds(j * LANES, LANES)
                x = hid[i, rows, cols].astype(jnp.float32).reshape(BLOCK // 8, 8, LANES)
                squares = squares + x * x
                products = products + x * scaled[:, cols][None]
            parts[i % 2, 0, rows, :] = squares.reshape(BLOCK, LANES)
            parts[i % 2, 1, rows, :] = products.reshape(BLOCK, LANES)

    part_copies = [
        pltpu.make_async_remote_copy(
            src_ref=part_send.at[k - 1],
            dst_ref=part_recv.at[k - 1],
            send_sem=near_sem,
            recv_sem=part_recv_sem.at[k - 1],
            device_id=(me_seq, lax.rem(me_ten + k, tensor_count)),
            device_id_type=pl.DeviceIdType.MESH,
        )
        for k in range(1, tensor_count)
    ]

    def send_column():
        def send(k, _):
            if mirrored:
                seq = me_seq
                for i in range(bits):
                    if (seq_count - k) >> i & 1:
                        seq = seq + flips[i]
            else:
                seq = lax.rem(me_seq + k, seq_count)
            pltpu.make_async_remote_copy(
                src_ref=board.at[my_slot, :, early_lanes],
                dst_ref=board.at[my_slot, :, early_lanes],
                send_sem=send_sem,
                recv_sem=early_recv_sem,
                device_id=(seq, me_ten),
                device_id_type=pl.DeviceIdType.MESH,
            ).start()
            return 0

        if unrolled:
            for k in range(1, seq_count):
                send(k, 0)
        else:
            lax.fori_loop(1, seq_count, send, 0)

    def forward_column():
        column = board.at[pl.ds(me_ten * seq_count, seq_count), :, early_lanes]
        for k in range(1, tensor_count):
            pltpu.make_async_remote_copy(
                src_ref=column,
                dst_ref=column,
                send_sem=send_sem,
                recv_sem=forward_recv_sem,
                device_id=(me_seq, lax.rem(me_ten + k, tensor_count)),
                device_id_type=pl.DeviceIdType.MESH,
            ).start()

    def send_all(lanes, recv_sem):
        def send(k, _):
            pltpu.make_async_remote_copy(
                src_ref=board.at[my_slot, :, lanes],
                dst_ref=board.at[my_slot, :, lanes],
                send_sem=send_sem,
                recv_sem=recv_sem,
                device_id=peer(k),
                device_id_type=pl.DeviceIdType.MESH,
            ).start()
            return 0

        each_peer(send)

    def blocks(count, lanes, sem):
        view = board.at[pl.ds(0, count), :, lanes]
        return pltpu.make_async_copy(view, view, sem)

    def publish():
        wait_group(far, far_sem)
        scalar_copies[2].wait()
        for r in range(own_rows):
            ratio = jnp.exp(newp[r : r + 1, :] - oldp[r : r + 1, :])
            weight = msk[r : r + 1, :].astype(jnp.float32)
            reward = jnp.broadcast_to(rew[pl.ds(first_row + r, 1), :], (8, length))
            rows_info[r].update(ratio=ratio, weight=weight, reward=reward)
            board[my_slot, r : r + 1, pl.ds(0, length)] = ratio
            board[my_slot, r : r + 1, weight_lanes] = weight
        send_column()

    squares_of = [[] for _ in range(seqs_all)]
    products_of = [[] for _ in range(seqs_all)]
    pending = []

    half = lambda axis: lax.broadcasted_iota(jnp.int32, (16, 2 * LANES), axis)
    pick = jnp.where((half(0) < 8) == (half(1) < LANES), 1.0, 0.0).astype(jnp.bfloat16)

    def flush():
        while pending:
            i, start, stop = pending.pop(0)
            rows = pl.ds(start, stop - start)
            squares = split(parts[i % 2, 0, rows, :], 2)
            products = split(parts[i % 2, 1, rows, :], 3)
            both = sum(lane_sums(pick, pair) for pair in zip(squares, products))
            both = both + lane_sums(pick[:, LANES:], products[2:])
            squares_of[i].append(both[0:8, :])
            products_of[i].append(both[8:16, :])

    partner_rows = seqs_all - own_rows
    for i in range(seqs_all):
        start = 0
        for c in range(chunks):
            hid_copy(i, c).wait()
            if i + ahead_rows < seqs_all:
                hid_copy(i + ahead_rows, c).start()
            if i > 0 and c == 1 and i <= partner_rows:
                k, r = divmod(i - 1, own_rows)
                squares = jnp.concatenate(squares_of[i - 1], axis=1)
                products = jnp.concatenate(products_of[i - 1], axis=1)
                part_send[k, 2 * r : 2 * r + 1, :] = squares[0:1, :]
                part_send[k, 2 * r + 1 : 2 * r + 2, :] = products[0:1, :]
            if i == partner_rows and c == 1:
                pl.semaphore_wait(barrier, devices - 1)
                for copy in part_copies:
                    copy.start()
            if i == partner_rows and c == 1:
                publish()
            if i < partner_rows or c in (0, chunks - 1):
                flush()
            add_chunk(i, c)
            done = (c + 1) * chunk
            if done == length or i >= partner_rows and done % LANES == 0:
                pending.append((i, start, done))
                start = done
    flush()
    for copy in part_copies:
        copy.wait_recv()
    if part_copies:
        pltpu.make_async_copy(part_send, part_send, near_sem).wait()

    for r in range(own_rows):
        trace, reward = rows_info[r]["trace"], rows_info[r]["reward"]
        squares = jnp.concatenate(squares_of[partner_rows + r], axis=1)
        products = jnp.concatenate(products_of[partner_rows + r], axis=1)
        for k in range(1, tensor_count):
            squares = squares + part_recv[k - 1, 2 * r : 2 * r + 1, :]
            products = products + part_recv[k - 1, 2 * r + 1 : 2 * r + 2, :]
        values = products * lax.rsqrt(squares / width + EPS_NORM)
        values_ref[r : r + 1, :] = values[0:1, :]
        pull = reward + (1.0 - trace) / trace * values
        rest, rows = pull, []
        for _ in range(PIECES):
            rows.append(rest.astype(jnp.bfloat16).astype(jnp.float32))
            rest = rest - rows[-1]
        rows = jnp.concatenate(rows + [rest], axis=0).astype(jnp.bfloat16)
        adv = -values / trace
        for n in range(PIECES):
            used = PIECES - n
            summed = lax.dot_general(
                rows[0 : 16 * pl.cdiv(used, 2), :],
                reach[n, r],
                (((1,), (0,)), ((), ())),
                preferred_element_type=jnp.float32,
            )
            for m in range(used):
                adv = adv + summed[8 * m : 8 * m + 8, :]
        board[my_slot, r : r + 1, adv_lanes] = adv[0:1, :]
        board[my_slot, r : r + 1, offset_lanes] = jnp.broadcast_to(
            values[0:1, 0:1] + trace[0:1, 0:1] * adv[0:1, 0:1], (1, LANES)
        )

    send_all(late_lanes, late_recv_sem)

    blocks(seq_count - 1, early_lanes, early_recv_sem).wait()
    forward_column()
    blocks(devices - seq_count, early_lanes, forward_recv_sem).wait()
    everyone = [
        (t * own_rows + r, pl.ds(t * seq_count, seq_count), r)
        for t in range(tensor_count)
        for r in range(own_rows)
    ]
    total = lambda x: jnp.sum(jnp.sum(x, axis=0, keepdims=True), axis=1, keepdims=True)
    def gather(slots, r, start):
        return jnp.concatenate(
            [board[slots, r, pl.ds(start + n, LANES)] for n in range(0, length, LANES)], axis=1
        )

    count = jnp.zeros((seq_count, length), jnp.float32)
    coefs, chains = [], []
    place = lax.broadcasted_iota(jnp.int32, (seq_count, LANES), 0)
    for row, slots, r in everyone:
        count = count + gather(slots, r, length)
        coef = coef_of(board[slots, r, done_lanes], row)
        coefs.append(coef)
        slope[slots, r, :] = jnp.broadcast_to(trc[row] * coef[:, 0:1], (seq_count, LANES))
        chain = [jnp.where(place == 0, 1.0, 0.0)]
        for n in range(1, seq_count):
            step = slope[slots.start + n, r : r + 1, :]
            chain.append(jnp.where(place == n, 1.0, chain[-1] * step))
        chains.append(chain)
    each = 1.0 / total(count)
    own_coefs = [coef_of(board[my_slot, r : r + 1, done_lanes], first_row + r) for r in range(own_rows)]
    blocks(devices - 1, late_lanes, late_recv_sem).wait()

    advs = []
    sums = jnp.zeros((seq_count, length), jnp.float32)
    for row, slots, r in everyone:
        terms = [boot[row] * chains[row][-1]]
        for n in range(1, seq_count):
            offset = board[slots.start + n, r : r + 1, offset_lanes]
            terms.append(chains[row][n - 1] * offset)
        while len(terms) > 1:
            terms = [sum(terms[n : n + 2]) for n in range(0, len(terms), 2)]
        carry[slots, r, :] = terms[0]
        entering = jnp.concatenate(terms * (length // LANES), axis=1)
        adv = gather(slots, r, adv_lanes.start) + coefs[row] * entering
        advs.append(adv)
        sums = sums + gather(slots, r, length) * adv
    mean = total(sums) * each

    def token_loss(ratio, weight, white):
        clipped = jnp.clip(ratio, 1.0 - CLIP, 1.0 + CLIP)
        return -weight * jnp.minimum(ratio * white, clipped * white)

    spread = jnp.zeros((seq_count, length), jnp.float32)
    losses = jnp.zeros((seq_count, length), jnp.float32)
    for row, slots, r in everyone:
        centred = advs[row] - mean
        weight = gather(slots, r, length)
        spread = spread + weight * centred * centred
        losses = losses + token_loss(gather(slots, r, 0), weight, centred)
    scale = lax.rsqrt(total(spread) * each + EPS_WHITE)
    loss_ref[...] = jnp.broadcast_to(total(losses) * each * scale, (1, LANES))

    for r in range(own_rows):
        entering = jnp.concatenate([carry[my_slot, r : r + 1, :]] * (length // LANES), axis=1)
        adv = board[my_slot, r : r + 1, adv_lanes] + own_coefs[r] * entering
        white = (adv - mean) * scale
        white_ref[r : r + 1, :] = white
        token_ref[r : r + 1, :] = token_loss(rows_info[r]["ratio"], rows_info[r]["weight"], white)

    view = board.at[pl.ds(0, devices - 1)]
    pltpu.make_async_copy(view, view, send_sem).wait()


def write_out(*refs):
    half = len(refs) // 2
    for src, dst in zip(refs[:half], refs[half:]):
        dst[...] = src[:, : dst.shape[1]]


def shards(seq_count, tensor_count, *args):
    seqs_all, length, local_width = args[0].shape
    own_rows = seqs_all // tensor_count
    devices = seq_count * tensor_count
    chunk = min(length, 64)
    f32 = jnp.float32
    row = jax.ShapeDtypeStruct((own_rows, length), f32)
    dma = pltpu.SemaphoreType.DMA
    others = max(tensor_count - 1, 1)
    shapes = [row, row, row, jax.ShapeDtypeStruct((1, 1), f32)]
    near_bytes = 2 * local_width * 2 + seqs_all * length * 4
    far_bytes = (3 * own_rows + seqs_all) * length * 4
    outs = pl.pallas_call(
        functools.partial(kernel, seq_count, tensor_count, local_width * tensor_count, chunk),
        out_shape=[row, row, row, jax.ShapeDtypeStruct((1, LANES), f32)],
        in_specs=[pl.BlockSpec(memory_space=pltpu.HBM)] * 11,
        out_specs=[pl.BlockSpec(memory_space=pltpu.VMEM)] * 4,
        scratch_shapes=[
            pltpu.VMEM((seqs_all, length, local_width), jnp.bfloat16),
            pltpu.VMEM((local_width,), jnp.bfloat16),
            pltpu.VMEM((local_width,), jnp.bfloat16),
            pltpu.VMEM((seqs_all, length), f32),
            pltpu.VMEM((seqs_all, length), jnp.int32),
            pltpu.VMEM((own_rows, length), jnp.int32),
            pltpu.VMEM((own_rows, length), f32),
            pltpu.VMEM((own_rows, length), f32),
            pltpu.SMEM((seqs_all,), f32),
            pltpu.SMEM((seqs_all,), f32),
            pltpu.SMEM((seqs_all,), f32),
            pltpu.VMEM((max(near_bytes, far_bytes) // (4 * LANES), 1, LANES), f32),
            pltpu.VMEM((8, local_width), f32),
            pltpu.VMEM((2, 2, length, LANES), f32),
            pltpu.VMEM((PIECES, own_rows, length, length), jnp.bfloat16),
            pltpu.VMEM((others, 2 * own_rows, length), f32),
            pltpu.VMEM((others, 2 * own_rows, length), f32),
            pltpu.VMEM((devices, own_rows, 3 * length + 2 * LANES), f32),
            pltpu.VMEM((devices, own_rows, LANES), f32),
            pltpu.VMEM((devices, own_rows, LANES), f32),
            dma((min(seqs_all, AHEAD_ROWS) * (length // chunk),)),
            dma,
            dma,
            dma((2,)),
            dma((others,)),
            dma,
            dma,
            dma,
            dma,
        ],
        compiler_params=pltpu.CompilerParams(
            collective_id=0, has_side_effects=True, vmem_limit_bytes=24 << 20
        ),
    )(*[pltpu.with_memory_space_constraint(x, pltpu.HBM) for x in args])
    outs = pl.pallas_call(
        write_out,
        out_shape=shapes,
        in_specs=[pl.BlockSpec(memory_space=pltpu.VMEM)] * 4,
        out_specs=[pl.BlockSpec(memory_space=pltpu.VMEM)] * 4,
        compiler_params=pltpu.CompilerParams(vmem_limit_bytes=1 << 20),
    )(*outs)
    return (outs[0], outs[1], outs[2], outs[3].reshape(()))


def solution(mesh):
    in_specs = (
        P(None, "seq", "tensor"),
        P("tensor"),
        P("tensor"),
        P(None, "seq"),
        P(None, "seq"),
        P("tensor", "seq"),
        P("tensor", "seq"),
        P("tensor", "seq"),
        P(),
        P(),
        P(),
    )
    out_specs = (P("tensor", "seq"), P("tensor", "seq"), P("tensor", "seq"), P())
    body = functools.partial(shards, mesh.shape["seq"], mesh.shape["tensor"])
    return jax.shard_map(body, mesh=mesh, in_specs=in_specs, out_specs=out_specs, check_vma=False)
```
